32 devices in a mesh: gx: 8 (over z, x), gy: 4 (over y, core).
Axes of the slice: x: 2, y: 2, z: 4, core: 2. Of those that a mesh axis runs over, the one named last changes fastest.
Arguments:
- orbitals: bfloat16 [20000, 200], P('gx'), may hold values from -6 to 6
- projector: bfloat16 [6016, 20000], P('gy', 'gx'), may hold values from -0.0390625 to 0.0390625
- integrals: bfloat16 [8, 6016, 6016], P('gx', 'gy'), may hold values from -1 to 1
Outputs:
- exchange_matrix: float32 [6016, 6016], P('gx', 'gy')
- exchange_orbitals: float32 [20000, 200], P('gx', 'gy')
- energy_mean: float32 [], replicated
- trace_mean: float32 [], replicated
The draws below stay inside these ranges and needn't reach their ends.
All inputs are finite; a program needn't handle non-finite values.
Results may differ from the reference program's by a relative error of at most 0.008.
Values may be sent and summed in bfloat16 or wider, within the bound.
A program may use at most 128 MiB of HBM per device.

```python
import jax
import jax.numpy as jnp
from jax import lax

NAO = 20000
NADM = 6016
NOCC = 200
NAUX = 8


def draw_integrals(key, part):
    keyed = jax.random.fold_in(key, 11)
    first = jax.random.fold_in(keyed, 0)
    shape = (NAUX, NADM, NADM)
    base = jax.random.normal(first, shape, jnp.float32)
    aux_scale = 0.5 + jnp.arange(NAUX, dtype=jnp.float32) / max(NAUX - 1, 1)
    row_scale = 0.5 + jnp.arange(NADM, dtype=jnp.float32) / max(NADM - 1, 1)
    sigma = (NADM * NOCC * NAUX) ** (-0.5)
    values = base * aux_scale[:, None, None] * row_scale[None, :, None] * sigma
    return jnp.clip(values, -1.0, 1.0).astype(jnp.bfloat16)


def block_scale(rng, shape, cuts, smallest, high):
    factor_of, own = 1.0, jax.random.fold_in(rng, 6)
    for axis_at, blocks in cuts:
        heights = jnp.exp(jax.random.uniform(jax.random.fold_in(own, axis_at), (blocks,), jnp.float32, smallest / len(cuts), high / len(cuts)))
        factor_of = factor_of * jnp.repeat(heights, shape[axis_at] // blocks).reshape([-1 if axis == axis_at else 1 for axis in range(len(shape))])
    return factor_of


def gaussian(rng, dims, width, reach, pieces=(), kind=jnp.bfloat16):
    gain = block_scale(rng, dims, pieces, -0.22, 0.18) if pieces else 1.0
    drawn = jax.random.normal(rng, dims, jnp.float32) * width * gain
    return jnp.minimum(jnp.maximum(drawn, -reach), reach).astype(kind)


def setup_inputs(seed: int = 0) -> dict:
    splits = jax.random.split(jax.random.key(seed), 4)
    return {
        "orbitals": gaussian(splits[0], (NAO, NOCC), 1.0, 6.0, ((0, 8),)),
        "projector": gaussian(splits[1], (NADM, NAO), NAO ** -0.5, 0.0390625, ((0, 4), (1, 8))),
        "integrals": draw_integrals(jax.random.fold_in(splits[3], 71), 0),
    }


def reference(orbitals, projector, integrals):
    admm = jnp.dot(projector, orbitals, preferred_element_type=jnp.float32).astype(jnp.bfloat16)

    def transform(slab):
        return jnp.dot(slab, admm, preferred_element_type=jnp.float32).astype(jnp.bfloat16)

    half = lax.map(transform, integrals)
    merged = jnp.transpose(half, (1, 0, 2)).reshape(NADM, NAUX * NOCC)
    exchange = jnp.dot(merged, merged.T, preferred_element_type=jnp.float32)
    admm_wide = admm.astype(jnp.float32)
    applied = jnp.dot(exchange, admm_wide, precision=lax.Precision.HIGHEST)
    applied_low = applied.astype(jnp.bfloat16)
    back = jnp.dot(projector.T, applied_low, preferred_element_type=jnp.float32)
    energy = -0.5 * jnp.sum(admm_wide * applied) / (NADM * NOCC)
    trace = jnp.sum(jnp.diagonal(exchange)) / NADM
    return exchange, back, energy, trace
```

```python
import functools
import types

import jax
import jax.numpy as jnp
from jax import lax
from jax.experimental import pallas as pl
from jax.experimental.pallas import tpu as pltpu
from jax.sharding import PartitionSpec as P

MESH = pl.DeviceIdType.MESH
LIMIT = 63 * 1024 * 1024
LANE = 128
SUB = 2
F32, BF16 = jnp.float32, jnp.bfloat16


def factor(size):
    inner = 1
    while inner * inner * 4 <= size:
        inner *= 2
    return size // inner, inner


def up(value, unit):
    return -(-value // unit) * unit


def remote(src, dst, send, recv, dev):
    return pltpu.make_async_remote_copy(
        src_ref=src, dst_ref=dst, send_sem=send, recv_sem=recv, device_id=dev, device_id_type=MESH
    )


def dot(a, b, dims):
    return lax.dot_general(a, b, (dims, ((), ())), preferred_element_type=F32)


def layout(size_x, size_y, rows, depth, occ):
    g = types.SimpleNamespace(size_x=size_x, size_y=size_y, rows=rows, depth=depth, occ=occ)
    g.nz, g.nx = factor(size_x)
    g.ny = size_y // 2
    g.total = rows * size_y
    g.lz = up(-(-rows // g.nz), LANE)
    g.rx = up(-(-occ // g.nx), 8)
    g.off = [min(i * g.rx, occ - g.rx) for i in range(g.nx)]
    g.wide = up(rows, SUB * LANE)
    g.own = max(g.wide, g.nz * g.lz)
    g.units = g.wide // LANE
    g.subs = g.units // SUB
    g.na = g.subs - 1
    g.slots = g.na + g.nx
    g.block = g.total // size_x
    g.per = size_x // size_y
    g.window = max(up(i * g.block % LANE + g.block, LANE) for i in range(g.per))
    g.wu = g.window // LANE
    g.firsts = [min(i * g.block // LANE * LANE, g.wide - g.window) for i in range(g.per)]
    g.share = occ // size_y
    g.j = up(g.share, 8)
    g.step = 512
    g.chunks = -(-depth // g.step)
    g.group = 512 if g.wide % 512 == 0 else 256
    return g


def greet(size_x, size_y):
    gx, gy = lax.axis_index("gx"), lax.axis_index("gy")
    barrier = pltpu.get_barrier_semaphore()

    def hello(step, carry):
        other = lax.rem(gx * size_y + gy + step, size_x * size_y)
        pl.semaphore_signal(
            barrier, inc=1, device_id=(other // size_y, lax.rem(other, size_y)), device_id_type=MESH
        )
        return carry

    lax.fori_loop(1, size_x * size_y, hello, 0)
    pl.semaphore_wait(barrier, size_x * size_y - 1)


def whole_kernel(g, names, *refs):
    r = types.SimpleNamespace(**dict(zip(names, refs)))
    nz, nx, ny, occ, rows = g.nz, g.nx, g.ny, g.occ, g.rows
    gx, gy = lax.axis_index("gx"), lax.axis_index("gy")
    z, x = gx // nx, lax.rem(gx, nx)
    y, c = gy // 2, lax.rem(gy, 2)
    partner = (gx, gy + 1 - 2 * c)

    loads = [pltpu.make_async_copy(r.orb_h, r.orbv, r.load_sem.at[0])]
    for i in range(nz):
        low, high = i * g.lz, min((i + 1) * g.lz, rows)
        if high > low:
            loads.append(
                pltpu.make_async_copy(r.proj_h.at[low:high], r.projv.at[low:high], r.load_sem.at[i + 1])
            )
    for load in loads:
        load.start()
    span = SUB * LANE

    def int_load(s):
        low, high = s * span, min((s + 1) * span, rows)
        return pltpu.make_async_copy(r.int_h.at[0, low:high], r.integ.at[low:high], r.int_sem.at[s])

    for s in range(g.subs):
        int_load(s).start()
    greet(g.size_x, g.size_y)
    for load in loads:
        load.wait()

    def x_part(zz, e):
        to = lax.rem(x + e, nx)
        return remote(
            r.part.at[zz, to], r.xland.at[e, zz], r.send_p.at[zz, e], r.recv_p.at[zz, e], (z * nx + to, gy)
        )

    def project(i, carry):
        zz = lax.rem(z + 1 + i, nz)
        rows_of = r.projv[pl.ds(pl.multiple_of(zz * g.lz, LANE), g.lz), :]
        value = dot(r.orbv[...], rows_of, ((0,), (1,)))
        for xx in range(nx):
            r.part[zz, xx] = value[g.off[xx]:g.off[xx] + g.rx].astype(BF16)
        for e in range(1, nx):
            x_part(zz, e).start()
        return carry

    lax.fori_loop(0, nz, project, 0)

    def x_sum(zz):
        value = r.part[zz, x].astype(F32)
        for e in range(1, nx):
            x_part(zz, e).wait_recv()
            value = value + r.xland[e, zz].astype(F32)
        return value

    def z_part(d):
        to = lax.rem(z + d, nz)
        return remote(r.zsum.at[d], r.zland.at[d], r.send_q.at[d], r.recv_q.at[d], (to * nx + x, gy))

    for d in range(1, nz):
        r.zsum[d] = x_sum(lax.rem(z + d, nz)).astype(BF16)
        z_part(d).start()
    total = x_sum(z)
    for d in range(1, nz):
        z_part(d).wait_recv()
        total = total + r.zland[d].astype(F32)
    r.agb[gy, gx] = total.astype(BF16)

    def at(d, e):
        return lax.rem(z - d + nz, nz) * nx + lax.rem(x - e + nx, nx)

    def group(f, core):
        return lax.rem(y - f + ny, ny) * 2 + core

    def block_z(d, came):
        ref = r.agb.at[gy, at(d, 0) if came else gx]
        return remote(ref, ref, r.send_az.at[d], r.recv_az.at[d], (lax.rem(z + d, nz) * nx + x, gy))

    def block_x(gg, q, slot, e):
        ref = r.agb.at[gg, q]
        return remote(ref, ref, r.send_ax.at[slot, e], r.recv_ax.at[slot, e], (z * nx + lax.rem(x + e, nx), gy))

    def block_y(gg, q, slot, f):
        ref = r.agb.at[gg, q]
        return remote(ref, ref, r.send_ay.at[slot, f], r.recv_ay.at[slot, f], (gx, lax.rem(y + f, ny) * 2 + c))

    def block_c(d, e, f, core):
        ref = r.agb.at[group(f, core), at(d, e)]
        slot = (f * nz + d) * nx + e
        return remote(ref, ref, r.send_ac.at[slot], r.recv_ac.at[slot], partner)

    for d in range(1, nz):
        block_z(d, False).start()

    @pl.when(c == 0)
    def _():
        for d in range(nz):
            if d > 0:
                block_z(d, True).wait_recv()
            for e in range(1, nx):
                block_x(gy, at(d, 0), d, e).start()
            for f in range(1, ny):
                block_y(gy, at(d, 0), d * nx, f).start()
            block_c(d, 0, 0, c).start()
        for d in range(nz):
            for e in range(1, nx):
                block_x(gy, at(d, e), d, e).wait_recv()
                for f in range(1, ny):
                    block_y(gy, at(d, e), d * nx + e, f).start()
                block_c(d, e, 0, c).start()
        for d in range(nz):
            for e in range(nx):
                for f in range(1, ny):
                    block_y(group(f, c), at(d, e), d * nx + e, f).wait_recv()
                    block_c(d, e, f, c).start()

    @pl.when(c == 1)
    def _():
        for d in range(nz):
            if d > 0:
                block_z(d, True).wait_recv()
            for f in range(1, ny):
                block_y(gy, at(d, 0), d, f).start()
            for e in range(1, nx):
                block_x(gy, at(d, 0), d * ny, e).start()
            block_c(d, 0, 0, c).start()
        for d in range(nz):
            for f in range(1, ny):
                block_y(group(f, c), at(d, 0), d, f).wait_recv()
                for e in range(1, nx):
                    block_x(group(f, c), at(d, 0), d * ny + f, e).start()
                block_c(d, 0, f, c).start()
        for d in range(nz):
            for f in range(ny):
                for e in range(1, nx):
                    block_x(group(f, c), at(d, e), d * ny + f, e).wait_recv()
                    block_c(d, e, f, c).start()

    for d in range(nz):
        for e in range(nx):
            for f in range(ny):
                block_c(d, e, f, 1 - c).wait_recv()

    lane = lax.broadcasted_iota(jnp.int32, (g.rx, g.lz), 1)
    for gg in range(g.size_y):
        for zz in range(nz):
            width = min(g.lz, rows - zz * g.lz)
            if width <= 0:
                continue
            base = gg * rows + zz * g.lz
            for xx in range(nx):
                r.admm[g.off[xx]:g.off[xx] + g.rx, base:base + width] = r.agb[gg, zz * nx + xx][:, :width]
    for zz in range(nz):
        for xx in range(nx):
            piece = r.agb[gy, zz * nx + xx]
            piece = jnp.where(lane + zz * g.lz < rows, piece.astype(F32), 0.0).astype(BF16)
            r.own[g.off[xx]:g.off[xx] + g.rx, zz * g.lz:(zz + 1) * g.lz] = piece

    devices = g.size_x * g.size_y
    me = gx * g.size_y + gy
    root = gx // g.per
    root_y, root_c = root // 2, lax.rem(root, 2)
    turn = lax.rem(gx, g.per)
    first = 0
    for i in range(g.per):
        first = jnp.where(turn == i, g.firsts[i] // LANE, first)
    mine = gy == root
    below = (y != root_y) & (c == root_c)
    last = c != root_c

    def part_of(zz, slot):
        if slot < g.na:
            return r.cols.at[zz * nx + x, pl.ds(SUB * slot, SUB)]
        return r.cols.at[zz * nx + slot - g.na, pl.ds(SUB * g.na, SUB)]

    def upward(k, slot):
        ref = part_of(jnp.maximum(z - k, 0), slot)
        return remote(ref, ref, r.send_u.at[k, slot], r.recv_u.at[k, slot], (jnp.minimum(z + 1, nz - 1) * nx + x, gy))

    def downward(k, slot):
        ref = part_of(jnp.minimum(z + k, nz - 1), slot)
        return remote(ref, ref, r.send_d.at[k, slot], r.recv_d.at[k, slot], (jnp.maximum(z - 1, 0) * nx + x, gy))

    def sideways(zz, sub, e, came):
        ref = r.cols.at[zz * nx + (lax.rem(x - e + nx, nx) if came else x), pl.ds(SUB * sub, SUB)]
        return remote(
            ref, ref, r.send_x.at[zz, sub, e], r.recv_x.at[zz, sub, e], (z * nx + lax.rem(x + e, nx), gy)
        )

    def row_y(q, unit, f):
        spot = unit - first
        return remote(
            r.cols.at[q, unit], r.rows.at[q, spot], r.send_y.at[q, spot, f], r.recv_y.at[q], (gx, lax.rem(y + f, ny) * 2 + c)
        )

    def row_c(q, unit):
        spot = unit - first
        return remote(r.cols.at[q, unit], r.rows.at[q, spot], r.send_c.at[q, spot], r.recv_c.at[q], partner)

    def row_all(q):
        return remote(r.rows.at[q], r.rows.at[q], r.send_w.at[q], r.recv_c.at[q], partner)

    def row_came(q):
        return remote(r.rows.at[q], r.rows.at[q], r.send_w.at[q], r.recv_y.at[q], partner)

    def row_own(q):
        return pltpu.make_async_copy(r.cols.at[q, pl.ds(first, g.wu)], r.rows.at[q], r.row_sem.at[q])

    def pass_rows(q, sub):
        for h in range(SUB):
            unit = sub * SUB + h

            @pl.when(mine & (unit >= first) & (unit < first + g.wu))
            def _():
                for f in range(1, ny):
                    row_y(q, unit, f).start()
                row_c(q, unit).start()

    r.mixed[...] = jnp.zeros_like(r.mixed)
    r.trace[...] = jnp.zeros_like(r.trace)
    for s in range(g.subs):
        int_load(s).wait()
    spots = lax.broadcasted_iota(jnp.int32, (occ, span), 1)

    def half(i, carry):
        s = lax.rem(i + g.na, g.subs)
        start = pl.multiple_of(s * span, span)
        value = dot(r.admm[...], r.integ[pl.ds(start, span), :], ((1,), (1,)))
        value = jnp.where(spots + start < rows, value, 0.0)
        low = value.astype(BF16)
        for h in range(SUB):
            r.cols[gx, SUB * s + h] = low[:, h * LANE:(h + 1) * LANE]

        @pl.when(i == 0)
        def _():
            for e in range(1, nx):
                sideways(z, g.na, e, False).start()

        @pl.when(i > 0)
        def _():
            ref = r.cols.at[gx, pl.ds(SUB * s, SUB)]

            @pl.when(z < nz - 1)
            def _():
                remote(ref, ref, r.send_u.at[0, s], r.recv_u.at[0, s], (jnp.minimum(z + 1, nz - 1) * nx + x, gy)).start()

            @pl.when(z > 0)
            def _():
                remote(ref, ref, r.send_d.at[0, s], r.recv_d.at[0, s], (jnp.maximum(z - 1, 0) * nx + x, gy)).start()

            for e in range(1, nx):
                sideways(z, s, e, False).start()

        for h in range(SUB):
            unit = SUB * s + h

            @pl.when(mine & (unit >= first) & (unit < first + g.wu))
            def _():
                for f in range(1, ny):
                    row_y(gx, unit, f).start()
                row_c(gx, unit).start()

        exact = low.astype(F32)
        r.trace[...] += jnp.sum(exact * exact, axis=0, keepdims=True)
        r.mixed[...] += dot(r.own[:, pl.ds(start, span)], low, ((1,), (1,)))
        return carry

    lax.fori_loop(0, g.subs, half, 0)

    def z_send(k, slot):
        @pl.when((z >= k) & (z < nz - 1))
        def _():
            upward(k, slot).start()

        @pl.when((z + k < nz) & (z > 0))
        def _():
            downward(k, slot).start()

    for e in range(nx):
        for xx in range(nx):
            @pl.when(lax.rem(x - e + nx, nx) == xx)
            def _(e=e, xx=xx):
                if e > 0:
                    sideways(z, g.na, e, True).wait_recv()
                    pass_rows(z * nx + xx, g.na)
                z_send(0, g.na + xx)

    low = r.mixed[...].astype(BF16)
    row_i = lax.broadcasted_iota(jnp.int32, (g.j, occ), 0)
    col_i = lax.broadcasted_iota(jnp.int32, (g.j, occ), 1)
    for gg in range(g.size_y):
        pick = ((row_i < g.share) & (col_i == row_i + gg * g.share)).astype(F32).astype(BF16)
        r.mpart[gg] = dot(pick, low, ((1,), (0,))).astype(BF16)

    def mix_y(d):
        to = lax.rem(gy + d, g.size_y)
        return remote(r.mpart.at[to], r.mland.at[d], r.send_m.at[d], r.recv_m.at[d], (gx, to))

    for d in range(1, g.size_y):
        mix_y(d).start()
    total = r.mpart[gy].astype(F32)
    for d in range(1, g.size_y):
        mix_y(d).wait_recv()
        total = total + r.mland[d].astype(F32)
    r.mall[gy, gx] = total.astype(BF16)

    def mix_x(d, came):
        ref = r.mall.at[gy, lax.rem(gx - d + g.size_x, g.size_x) if came else gx]
        return remote(ref, ref, r.send_n.at[d], r.recv_n.at[d], (lax.rem(gx + d, g.size_x), gy))

    def mix_share(f, came):
        ref = r.mall.at[group(f, c) if came else gy]
        return remote(ref, ref, r.send_o.at[f], r.recv_o.at[f], (gx, lax.rem(y + f, ny) * 2 + c))

    def mix_core(f, core):
        ref = r.mall.at[group(f, core)]
        return remote(ref, ref, r.send_r.at[f], r.recv_r.at[f], partner)

    for d in range(1, g.size_x):
        mix_x(d, False).start()
    stat_lane = lax.broadcasted_iota(jnp.int32, (8, LANE), 1)
    energy_part, trace_part = jnp.sum(total * total), jnp.sum(r.trace[...])
    r.stats[...] = jnp.where(stat_lane == 0, energy_part, jnp.where(stat_lane == 1, trace_part, 0.0))

    def stat_copy(slot, step, to):
        return remote(
            r.stats, r.sland.at[slot], r.send_s.at[step], r.recv_s.at[slot], (to // g.size_y, lax.rem(to, g.size_y))
        )

    def tell(step, carry):
        stat_copy(me, step, lax.rem(me + step, devices)).start()
        return carry

    lax.fori_loop(1, devices, tell, 0)

    r.acc[...] = jnp.zeros_like(r.acc)
    r.applied[...] = jnp.zeros_like(r.applied)

    def units(ref, q, low, high):
        return jnp.concatenate([ref[q, u] for u in range(low, high)], axis=1)

    def exchange_term(q):
        @pl.when(mine)
        def _():
            row_own(q).wait()

        @pl.when(below)
        def _():
            row_came(q).wait_recv()
            row_all(q).start()

        @pl.when(last)
        def _():
            row_all(q).wait_recv()

        left = units(r.rows, q, 0, g.wu)
        for low in range(0, g.wide, g.group):
            right = units(r.cols, q, low // LANE, (low + g.group) // LANE)
            r.acc[:, low:low + g.group] += dot(left, right, ((0,), (0,)))

    def applied_term(q):
        right = units(r.cols, q, 0, g.units)
        for gg in range(g.size_y):
            r.applied[gg * g.j:(gg + 1) * g.j, :] += dot(r.mall[gg, q], right, ((1,), (0,)))

    def level(k, act):
        def one(i, carry):
            zz = z + jnp.where(i < nx, -k, k)

            @pl.when((zz >= 0) & (zz < nz))
            def _():
                act(zz * nx + lax.rem(x + lax.rem(i, nx), nx))

            return carry

        lax.fori_loop(0, 2 * nx if k else nx, one, 0)

    def arrive_x(k):
        for side in ((-1, 1) if k else (1,)):
            zz = z + side * k

            @pl.when((zz >= 0) & (zz < nz))
            def _(zz=zz):
                zz = jnp.clip(zz, 0, nz - 1)
                for sub in range(g.na):
                    for e in range(1, nx):
                        sideways(zz, sub, e, True).wait_recv()
                        pass_rows(zz * nx + lax.rem(x - e + nx, nx), sub)

        def own_rows(q):
            @pl.when(mine)
            def _():
                row_own(q).start()

        level(k, own_rows)

    def arrive_z(k, slot):
        for up_way in (True, False):
            zz = z - k if up_way else z + k

            @pl.when((zz >= 0) & (zz < nz))
            def _(zz=zz, up_way=up_way):
                zz = jnp.clip(zz, 0, nz - 1)
                sems = (r.send_u, r.recv_u) if up_way else (r.send_d, r.recv_d)
                ref = part_of(zz, slot)
                remote(ref, ref, sems[0].at[k - 1, slot], sems[1].at[k - 1, slot], partner).wait_recv()
                if k < nz - 1:
                    @pl.when((z < nz - 1) if up_way else (z > 0))
                    def _():
                        (upward if up_way else downward)(k, slot).start()
                if slot < g.na:
                    for e in range(1, nx):
                        sideways(zz, slot, e, False).start()
                    pass_rows(zz * nx + x, slot)
                else:
                    pass_rows(zz * nx + slot - g.na, g.na)

    for k in range(1, nz):
        for slot in range(g.slots):
            arrive_z(k, slot)
            if slot == min(2, g.slots - 1):
                arrive_x(k - 1)
            if slot == g.slots - 2:
                if k == 2:
                    for f in range(ny):
                        if f > 0:
                            mix_share(f, True).wait_recv()
                            mix_core(f, c).start()
                    for f in range(ny):
                        mix_core(f, 1 - c).wait_recv()
                    level(0, applied_term)
                level(k - 1, exchange_term)
                if k >= 2:
                    level(k - 1, applied_term)
        if k == 1:
            for d in range(1, g.size_x):
                mix_x(d, True).wait_recv()
            for f in range(1, ny):
                mix_share(f, False).start()
            mix_core(0, c).start()
    arrive_x(nz - 1)
    level(nz - 1, applied_term)

    low = r.applied[:, :rows].astype(BF16)

    def back_c(n, core):
        return remote(r.bpart.at[n, core], r.bland.at[n], r.send_v.at[n], r.recv_v.at[n], partner)

    def back_y(n, f):
        to = lax.rem(y + f, ny)
        return remote(r.bsum.at[n, to], r.byland.at[n, f], r.send_b.at[n, f], r.recv_b.at[n, f], (gx, to * 2 + c))

    for n in range(g.chunks):
        start, stop = n * g.step, min((n + 1) * g.step, g.depth)
        value = dot(low, r.projv[:rows, start:stop], ((1,), (0,)))
        for gg in range(g.size_y):
            r.bpart[n, gg % 2, gg // 2, :, :stop - start] = value[gg * g.j:(gg + 1) * g.j].astype(BF16)
        back_c(n, 1 - c).start()
    for n in range(g.chunks):
        back_c(n, 1 - c).wait_recv()
        total = r.bpart[n, c].astype(F32) + r.bland[n].astype(F32)
        r.bsum[n] = total.astype(BF16)
        for f in range(1, ny):
            back_y(n, f).start()
    level(nz - 1, exchange_term)
    for i in range(g.per):
        begin = i * g.block - g.firsts[i]

        @pl.when(turn == i)
        def _(begin=begin):
            r.exch[...] = r.acc[begin:begin + g.block, :rows]

    for n in range(g.chunks):
        total = r.bpart[n, c, y].astype(F32) + r.bland[n, y].astype(F32)
        for f in range(1, ny):
            back_y(n, f).wait_recv()
            total = total + r.byland[n, f].astype(F32)
        r.back[:, n * g.step:(n + 1) * g.step] = total

    def hear(step, carry):
        stat_copy(lax.rem(me + step, devices), step, me).wait_recv()
        return carry

    lax.fori_loop(1, devices, hear, 0)
    r.sland[me] = r.stats[...]
    r.sums[...] = jnp.sum(r.sland[...], axis=0)

    def told(step, carry):
        stat_copy(me, step, me).wait_send()
        return carry

    lax.fori_loop(1, devices, told, 0)
    for zz in range(nz):
        for e in range(1, nx):
            x_part(zz, e).wait_send()
    for d in range(1, nz):
        z_part(d).wait_send()
        block_z(d, False).wait_send()

    @pl.when(c == 0)
    def _():
        for d in range(nz):
            for e in range(1, nx):
                block_x(gy, at(d, 0), d, e).wait_send()
            for e in range(nx):
                for f in range(1, ny):
                    block_y(gy, at(d, e), d * nx + e, f).wait_send()

    @pl.when(c == 1)
    def _():
        for d in range(nz):
            for f in range(1, ny):
                block_y(gy, at(d, 0), d, f).wait_send()
            for f in range(ny):
                for e in range(1, nx):
                    block_x(group(f, c), at(d, 0), d * ny + f, e).wait_send()

    for d in range(nz):
        for e in range(nx):
            for f in range(ny):
                block_c(d, e, f, c).wait_send()
    for k in range(nz - 1):
        for slot in range(g.slots):
            @pl.when((z >= k) & (z < nz - 1))
            def _(k=k, slot=slot):
                upward(k, slot).wait_send()

            @pl.when((z + k < nz) & (z > 0))
            def _(k=k, slot=slot):
                downward(k, slot).wait_send()
    for e in range(1, nx):
        for zz in range(nz):
            for sub in range(g.na):
                sideways(zz, sub, e, False).wait_send()
        sideways(z, g.na, e, False).wait_send()

    def drain(q, carry):
        @pl.when(mine)
        def _():
            for spot in range(g.wu):
                for f in range(1, ny):
                    row_y(q, first + spot, f).wait_send()
                row_c(q, first + spot).wait_send()

        @pl.when(below)
        def _():
            row_all(q).wait_send()

        return carry

    lax.fori_loop(0, g.size_x, drain, 0)
    for d in range(1, g.size_y):
        mix_y(d).wait_send()
    for d in range(1, g.size_x):
        mix_x(d, False).wait_send()
    for f in range(1, ny):
        mix_share(f, False).wait_send()
    for f in range(ny):
        mix_core(f, c).wait_send()
    for n in range(g.chunks):
        back_c(n, 1 - c).wait_send()
        for f in range(1, ny):
            back_y(n, f).wait_send()


def whole(g, orbitals, projector, integrals):
    dma, vmem = pltpu.SemaphoreType.DMA, pltpu.VMEM
    nz, nx, ny, occ = g.nz, g.nx, g.ny, g.occ
    devices = g.size_x * g.size_y
    scratch = dict(
        orbv=vmem(orbitals.shape, BF16),
        projv=vmem((max(nz * g.lz, g.rows), g.depth), BF16),
        integ=vmem((g.wide, g.total), BF16),
        part=vmem((nz, nx, g.rx, g.lz), BF16),
        xland=vmem((nx, nz, g.rx, g.lz), BF16),
        zsum=vmem((nz, g.rx, g.lz), BF16),
        zland=vmem((nz, g.rx, g.lz), BF16),
        agb=vmem((g.size_y, g.size_x, g.rx, g.lz), BF16),
        admm=vmem((occ, g.total), BF16),
        own=vmem((occ, g.own), BF16),
        cols=vmem((g.size_x, g.units, occ, LANE), BF16),
        rows=vmem((g.size_x, g.wu, occ, LANE), BF16),
        acc=vmem((g.window, g.wide), F32),
        mixed=vmem((occ, occ), F32),
        trace=vmem((1, SUB * LANE), F32),
        mpart=vmem((g.size_y, g.j, occ), BF16),
        mland=vmem((g.size_y, g.j, occ), BF16),
        mall=vmem((g.size_y, g.size_x, g.j, occ), BF16),
        stats=vmem((8, LANE), F32),
        sland=vmem((devices, 8, LANE), F32),
        applied=vmem((g.size_y * g.j, g.wide), F32),
        bpart=vmem((g.chunks, 2, ny, g.j, g.step), BF16),
        bland=vmem((g.chunks, ny, g.j, g.step), BF16),
        bsum=vmem((g.chunks, ny, g.j, g.step), BF16),
        byland=vmem((g.chunks, ny, g.j, g.step), BF16),
        load_sem=dma((nz + 1,)),
        int_sem=dma((g.subs,)),
        row_sem=dma((g.size_x,)),
    )
    for letter, shape in dict(
        p=(nz, nx), q=(nz,), az=(nz,), ax=(nz * ny, nx), ay=(nz * nx, ny), ac=(nz * nx * ny,),
        u=(nz, g.slots), d=(nz, g.slots), x=(nz, g.subs, nx), m=(g.size_y,), n=(g.size_x,), o=(ny,), r=(ny,),
        s=(devices,), v=(g.chunks,), b=(g.chunks, ny),
    ).items():
        scratch["send_" + letter] = dma(shape)
        scratch["recv_" + letter] = dma(shape)
    scratch.update(
        send_y=dma((g.size_x, g.wu, ny)), recv_y=dma((g.size_x,)), send_c=dma((g.size_x, g.wu)),
        recv_c=dma((g.size_x,)), send_w=dma((g.size_x,)),
    )
    names = ["orb_h", "proj_h", "int_h", "exch", "back", "sums"] + list(scratch)
    return pl.pallas_call(
        functools.partial(whole_kernel, g, names),
        out_shape=(
            jax.ShapeDtypeStruct((g.block, g.rows), F32),
            jax.ShapeDtypeStruct((g.j, g.chunks * g.step), F32),
            jax.ShapeDtypeStruct((8, LANE), F32),
        ),
        in_specs=[pl.BlockSpec(memory_space=pl.ANY)] * 3,
        out_specs=[pl.BlockSpec(memory_space=pltpu.VMEM)] * 3,
        scratch_shapes=list(scratch.values()),
        compiler_params=pltpu.CompilerParams(collective_id=1, has_side_effects=True, vmem_limit_bytes=LIMIT),
    )(orbitals, projector, integrals)


def on_device(size_x, size_y, orbitals, projector, integrals):
    g = layout(size_x, size_y, projector.shape[0], projector.shape[1], orbitals.shape[1])
    exchange, back, sums = whole(g, orbitals, projector, integrals)
    energy_mean = -0.5 * sums[0, 0] / (g.total * g.occ)
    trace_mean = sums[0, 1] / g.total
    return (exchange, back[:g.share, :g.depth].T, energy_mean, trace_mean)


def solution(mesh):
    return jax.shard_map(
        functools.partial(on_device, mesh.shape["gx"], mesh.shape["gy"]),
        mesh=mesh,
        in_specs=(P("gx", None), P("gy", "gx"), P("gx", "gy", None)),
        out_specs=(P("gx", "gy"), P("gx", "gy"), P(), P()),
        check_vma=False,
    )
```

```python
import functools
import types

import jax
import jax.numpy as jnp
from jax import lax
from jax.experimental import pallas as pl
from jax.experimental.pallas import tpu as pltpu
from jax.sharding import PartitionSpec as P

MESH = pl.DeviceIdType.MESH
LIMIT = 57 * 1024 * 1024
LANE = 128
SUB = 2
F32, BF16 = jnp.float32, jnp.bfloat16


def factor(size):
    inner = 1
    while inner * inner * 4 <= size:
        inner *= 2
    return size // inner, inner


def up(value, unit):
    return -(-value // unit) * unit


def remote(src, dst, send, recv, dev):
    return pltpu.make_async_remote_copy(
        src_ref=src, dst_ref=dst, send_sem=send, recv_sem=recv, device_id=dev, device_id_type=MESH
    )


def dot(a, b, dims):
    return lax.dot_general(a, b, (dims, ((), ())), preferred_element_type=F32)


def layout(size_x, size_y, rows, depth, occ):
    g = types.SimpleNamespace(size_x=size_x, size_y=size_y, rows=rows, depth=depth, occ=occ)
    g.nz, g.nx = factor(size_x)
    g.ny = size_y // 2
    g.total = rows * size_y
    g.lz = up(-(-rows // g.nz), LANE)
    g.rx = up(-(-occ // g.nx), 8)
    g.off = [min(i * g.rx, occ - g.rx) for i in range(g.nx)]
    g.wide = up(rows, SUB * LANE)
    g.own = max(g.wide, g.nz * g.lz)
    g.units = g.wide // LANE
    g.subs = g.units // SUB
    g.na = g.subs - 1
    g.slots = g.na + g.nx
    g.block = g.total // size_x
    g.per = size_x // size_y
    g.window = max(up(i * g.block % LANE + g.block, LANE) for i in range(g.per))
    g.wu = g.window // LANE
    g.firsts = [min(i * g.block // LANE * LANE, g.wide - g.window) for i in range(g.per)]
    g.share = occ // size_y
    g.j = up(g.share, 8)
    g.step = 512
    g.chunks = -(-depth // g.step)
    g.group = 512 if g.wide % 512 == 0 else 256
    return g


def flip(value, mask, size):
    if size & (size - 1):
        return lax.rem(value + mask, size)
    bit = 1
    while bit < size:
        if mask & bit:
            value = value + bit - 2 * bit * lax.rem(value // bit, 2)
        bit *= 2
    return value


def unflip(value, mask, size):
    return lax.rem(value - mask + size, size) if size & (size - 1) else flip(value, mask, size)


def greet(size_x, size_y):
    gx, gy = lax.axis_index("gx"), lax.axis_index("gy")
    barrier = pltpu.get_barrier_semaphore()

    def hello(step, carry):
        other = lax.rem(gx * size_y + gy + step, size_x * size_y)
        pl.semaphore_signal(
            barrier, inc=1, device_id=(other // size_y, lax.rem(other, size_y)), device_id_type=MESH
        )
        return carry

    lax.fori_loop(1, size_x * size_y, hello, 0)
    pl.semaphore_wait(barrier, size_x * size_y - 1)


def whole_kernel(g, names, *refs):
    r = types.SimpleNamespace(**dict(zip(names, refs)))
    nz, nx, ny, occ, rows = g.nz, g.nx, g.ny, g.occ, g.rows
    gx, gy = lax.axis_index("gx"), lax.axis_index("gy")
    z, x = gx // nx, lax.rem(gx, nx)
    y, c = gy // 2, lax.rem(gy, 2)
    partner = (gx, gy + 1 - 2 * c)

    loads = [pltpu.make_async_copy(r.orb_h, r.orbv, r.load_sem.at[0])]
    pieces = r.load_sem.shape[0] - 1
    tall = up(-(-g.depth // pieces), 8)
    for i in range(pieces):
        low, high = i * tall, min((i + 1) * tall, g.depth)
        loads.append(pltpu.make_async_copy(r.proj_h.at[low:high], r.projv.at[low:high], r.load_sem.at[i + 1]))
    for load in loads:
        load.start()
    span = SUB * LANE

    def int_load(s):
        low, high = s * span, min((s + 1) * span, rows)
        return pltpu.make_async_copy(r.int_h.at[0, low:high], r.integ.at[low:high], r.int_sem.at[s])

    greet(g.size_x, g.size_y)
    for load in loads:
        load.wait()
    for s in range(g.subs):
        int_load(s).start()

    def x_part(zz, e):
        to = lax.rem(x + e, nx)
        return remote(
            r.part.at[zz, to], r.xland.at[e, zz], r.send_p.at[zz, e], r.recv_p.at[zz, e], (z * nx + to, gy)
        )

    tail = (rows - 1) // g.lz

    def put(zz, value):
        for xx in range(nx):
            r.part[zz, xx, :, :value.shape[1]] = value[g.off[xx]:g.off[xx] + g.rx].astype(BF16)

    for d in reversed(range(nz)):
        zz = flip(z, d, nz)

        @pl.when(zz < tail)
        def _(zz=zz):
            put(zz, dot(r.orbv[...], r.projv[:, pl.ds(pl.multiple_of(zz * g.lz, LANE), g.lz)], ((1,), (0,))))

        @pl.when(zz == tail)
        def _():
            put(tail, dot(r.orbv[...], r.projv[:, tail * g.lz:rows], ((1,), (0,))))

        for e in range(1, nx):
            x_part(zz, e).start()

    def x_sum(zz):
        value = r.part[zz, x].astype(F32)
        for e in range(1, nx):
            x_part(zz, e).wait_recv()
            value = value + r.xland[e, zz].astype(F32)
        return value

    def z_part(d):
        return remote(r.zsum.at[d], r.zland.at[d], r.send_q.at[d], r.recv_q.at[d], (flip(z, d, nz) * nx + x, gy))

    for d in reversed(range(1, nz)):
        r.zsum[d] = x_sum(flip(z, d, nz)).astype(BF16)
        z_part(d).start()
    total = x_sum(z)
    for d in range(1, nz):
        z_part(d).wait_recv()
        total = total + r.zland[d].astype(F32)
    r.agb[gy, gx] = total.astype(BF16)

    def at(d, e):
        return unflip(z, d, nz) * nx + lax.rem(x - e + nx, nx)

    def group(f, core):
        return lax.rem(y - f + ny, ny) * 2 + core

    def block_z(d, came):
        ref = r.agb.at[gy, at(d, 0) if came else gx]
        return remote(ref, ref, r.send_az.at[d], r.recv_az.at[d], (flip(z, d, nz) * nx + x, gy))

    def block_x(gg, q, slot, e):
        ref = r.agb.at[gg, q]
        return remote(ref, ref, r.send_ax.at[slot, e], r.recv_ax.at[slot, e], (z * nx + lax.rem(x + e, nx), gy))

    def block_y(gg, q, slot, f):
        ref = r.agb.at[gg, q]
        return remote(ref, ref, r.send_ay.at[slot, f], r.recv_ay.at[slot, f], (gx, lax.rem(y + f, ny) * 2 + c))

    def block_c(d, e, f, core):
        ref = r.agb.at[group(f, core), at(d, e)]
        slot = (f * nz + d) * nx + e
        return remote(ref, ref, r.send_ac.at[slot], r.recv_ac.at[slot], partner)

    for d in range(1, nz):
        block_z(d, False).start()

    @pl.when(c == 0)
    def _():
        for d in range(nz):
            if d > 0:
                block_z(d, True).wait_recv()
            for e in range(1, nx):
                block_x(gy, at(d, 0), d, e).start()
            for f in range(1, ny):
                block_y(gy, at(d, 0), d * nx, f).start()
            block_c(d, 0, 0, c).start()
        for d in range(nz):
            for e in range(1, nx):
                block_x(gy, at(d, e), d, e).wait_recv()
                for f in range(1, ny):
                    block_y(gy, at(d, e), d * nx + e, f).start()
                block_c(d, e, 0, c).start()
        for d in range(nz):
            for e in range(nx):
                for f in range(1, ny):
                    block_y(group(f, c), at(d, e), d * nx + e, f).wait_recv()
                    block_c(d, e, f, c).start()

    @pl.when(c == 1)
    def _():
        for d in range(nz):
            if d > 0:
                block_z(d, True).wait_recv()
            for f in range(1, ny):
                block_y(gy, at(d, 0), d, f).start()
            for e in range(1, nx):
                block_x(gy, at(d, 0), d * ny, e).start()
            block_c(d, 0, 0, c).start()
        for d in range(nz):
            for f in range(1, ny):
                block_y(group(f, c), at(d, 0), d, f).wait_recv()
                for e in range(1, nx):
                    block_x(group(f, c), at(d, 0), d * ny + f, e).start()
                block_c(d, 0, f, c).start()
        for d in range(nz):
            for f in range(ny):
                for e in range(1, nx):
                    block_x(group(f, c), at(d, e), d * ny + f, e).wait_recv()
                    block_c(d, e, f, c).start()

    for d in range(nz):
        for e in range(nx):
            for f in range(ny):
                block_c(d, e, f, 1 - c).wait_recv()

    lane = lax.broadcasted_iota(jnp.int32, (g.rx, g.lz), 1)
    for gg in range(g.size_y):
        for zz in range(nz):
            width = min(g.lz, rows - zz * g.lz)
            if width <= 0:
                continue
            base = gg * rows + zz * g.lz
            for xx in range(nx):
                r.admm[g.off[xx]:g.off[xx] + g.rx, base:base + width] = r.agb[gg, zz * nx + xx][:, :width]
    for zz in range(nz):
        for xx in range(nx):
            piece = r.agb[gy, zz * nx + xx]
            piece = jnp.where(lane + zz * g.lz < rows, piece.astype(F32), 0.0).astype(BF16)
            r.own[g.off[xx]:g.off[xx] + g.rx, zz * g.lz:(zz + 1) * g.lz] = piece

    devices = g.size_x * g.size_y
    me = gx * g.size_y + gy
    root = gx // g.per
    root_y, root_c = root // 2, lax.rem(root, 2)
    turn = lax.rem(gx, g.per)
    first = 0
    for i in range(g.per):
        first = jnp.where(turn == i, g.firsts[i] // LANE, first)
    mine = gy == root
    below = (y != root_y) & (c == root_c)
    last = c != root_c

    def part_of(zz, slot):
        if slot < g.na:
            return r.cols.at[zz * nx + x, pl.ds(SUB * slot, SUB)]
        return r.cols.at[zz * nx + slot - g.na, pl.ds(SUB * g.na, SUB)]

    def upward(k, slot):
        ref = part_of(jnp.maximum(z - k, 0), slot)
        return remote(ref, ref, r.send_u.at[k, slot], r.recv_u.at[k, slot], (jnp.minimum(z + 1, nz - 1) * nx + x, gy))

    def downward(k, slot):
        ref = part_of(jnp.minimum(z + k, nz - 1), slot)
        return remote(ref, ref, r.send_d.at[k, slot], r.recv_d.at[k, slot], (jnp.maximum(z - 1, 0) * nx + x, gy))

    def sideways(zz, sub, e, came):
        ref = r.cols.at[zz * nx + (lax.rem(x - e + nx, nx) if came else x), pl.ds(SUB * sub, SUB)]
        return remote(
            ref, ref, r.send_x.at[zz, sub, e], r.recv_x.at[zz, sub, e], (z * nx + lax.rem(x + e, nx), gy)
        )

    def row_y(q, unit, f):
        spot = unit - first
        return remote(
            r.cols.at[q, unit], r.rows.at[q, spot], r.send_y.at[q, f], r.recv_y.at[q], (gx, lax.rem(y + f, ny) * 2 + c)
        )

    def row_c(q, unit):
        spot = unit - first
        return remote(r.cols.at[q, unit], r.rows.at[q, spot], r.send_c.at[q], r.recv_c.at[q], partner)

    def row_y_all(q, f):
        return remote(r.rows.at[q], r.rows.at[q], r.send_y.at[q, f], r.recv_y.at[q], partner)

    def row_c_all(q):
        return remote(r.rows.at[q], r.rows.at[q], r.send_c.at[q], r.recv_c.at[q], partner)

    def row_all(q):
        return remote(r.rows.at[q], r.rows.at[q], r.send_w.at[q], r.recv_c.at[q], partner)

    def row_came(q):
        return remote(r.rows.at[q], r.rows.at[q], r.send_w.at[q], r.recv_y.at[q], partner)

    def row_own(q):
        return pltpu.make_async_copy(r.cols.at[q, pl.ds(first, g.wu)], r.rows.at[q], r.row_sem.at[q])

    def pass_rows(q, sub):
        for h in range(SUB):
            unit = sub * SUB + h

            @pl.when(mine & (unit >= first) & (unit < first + g.wu))
            def _():
                for f in range(1, ny):
                    row_y(q, unit, f).start()
                row_c(q, unit).start()

    r.mixed[...] = jnp.zeros_like(r.mixed)
    r.trace[...] = jnp.zeros_like(r.trace)
    for s in range(g.subs):
        int_load(s).wait()
    spots = lax.broadcasted_iota(jnp.int32, (occ, span), 1)

    def half(i, carry):
        s = lax.rem(i + g.na, g.subs)
        start = pl.multiple_of(s * span, span)
        value = dot(r.admm[...], r.integ[pl.ds(start, span), :], ((1,), (1,)))
        value = jnp.where(spots + start < rows, value, 0.0)
        low = value.astype(BF16)
        for h in range(SUB):
            r.cols[gx, SUB * s + h] = low[:, h * LANE:(h + 1) * LANE]

        @pl.when(i == 0)
        def _():
            for e in range(1, nx):
                sideways(z, g.na, e, False).start()

        @pl.when(i > 0)
        def _():
            ref = r.cols.at[gx, pl.ds(SUB * s, SUB)]

            @pl.when(z < nz - 1)
            def _():
                remote(ref, ref, r.send_u.at[0, s], r.recv_u.at[0, s], (jnp.minimum(z + 1, nz - 1) * nx + x, gy)).start()

            @pl.when(z > 0)
            def _():
                remote(ref, ref, r.send_d.at[0, s], r.recv_d.at[0, s], (jnp.maximum(z - 1, 0) * nx + x, gy)).start()

            for e in range(1, nx):
                sideways(z, s, e, False).start()

        for h in range(SUB):
            unit = SUB * s + h

            @pl.when(mine & (unit >= first) & (unit < first + g.wu))
            def _():
                for f in range(1, ny):
                    row_y(gx, unit, f).start()
                row_c(gx, unit).start()

        exact = low.astype(F32)
        r.trace[...] += jnp.sum(exact * exact, axis=0, keepdims=True)
        r.mixed[...] += dot(r.own[:, pl.ds(start, span)], low, ((1,), (1,)))
        return carry

    lax.fori_loop(0, g.subs, half, 0)

    def z_send(k, slot):
        @pl.when((z >= k) & (z < nz - 1))
        def _():
            upward(k, slot).start()

        @pl.when((z + k < nz) & (z > 0))
        def _():
            downward(k, slot).start()

    for e in range(nx):
        for xx in range(nx):
            @pl.when(lax.rem(x - e + nx, nx) == xx)
            def _(e=e, xx=xx):
                if e > 0:
                    sideways(z, g.na, e, True).wait_recv()
                    pass_rows(z * nx + xx, g.na)
                z_send(0, g.na + xx)

    low = r.mixed[...].astype(BF16)
    row_i = lax.broadcasted_iota(jnp.int32, (g.j, occ), 0)
    col_i = lax.broadcasted_iota(jnp.int32, (g.j, occ), 1)
    for gg in range(g.size_y):
        pick = ((row_i < g.share) & (col_i == row_i + gg * g.share)).astype(F32).astype(BF16)
        r.mpart[gg] = dot(pick, low, ((1,), (0,))).astype(BF16)

    def mix_y(d):
        to = lax.rem(gy + d, g.size_y)
        return remote(r.mpart.at[to], r.mland.at[d], r.send_m.at[d], r.recv_m.at[d], (gx, to))

    for d in range(1, g.size_y):
        mix_y(d).start()
    total = r.mpart[gy].astype(F32)
    for d in range(1, g.size_y):
        mix_y(d).wait_recv()
        total = total + r.mland[d].astype(F32)
    r.mall[gy, gx] = total.astype(BF16)

    def mix_x(d, came):
        ref = r.mall.at[gy, lax.rem(gx - d + g.size_x, g.size_x) if came else gx]
        return remote(ref, ref, r.send_n.at[d], r.recv_n.at[d], (lax.rem(gx + d, g.size_x), gy))

    def mix_share(f, came):
        ref = r.mall.at[group(f, c) if came else gy]
        return remote(ref, ref, r.send_o.at[f], r.recv_o.at[f], (gx, lax.rem(y + f, ny) * 2 + c))

    def mix_core(f, core):
        ref = r.mall.at[group(f, core)]
        return remote(ref, ref, r.send_r.at[f], r.recv_r.at[f], partner)

    for d in range(1, g.size_x):
        mix_x(d, False).start()
    stat_lane = lax.broadcasted_iota(jnp.int32, (1, LANE), 1)
    energy_part, trace_part = jnp.sum(total * total), jnp.sum(r.trace[...])
    r.stats[...] = jnp.where(stat_lane == 0, energy_part, jnp.where(stat_lane == 1, trace_part, 0.0))

    def stat_copy(slot, step, to):
        return remote(
            r.stats, r.sland.at[slot], r.send_s.at[step], r.recv_s.at[slot], (to // g.size_y, lax.rem(to, g.size_y))
        )

    def tell(step, carry):
        stat_copy(me, step, lax.rem(me + step, devices)).start()
        return carry

    lax.fori_loop(1, devices, tell, 0)

    r.exch[...] = jnp.zeros_like(r.exch)
    r.applied[...] = jnp.zeros_like(r.applied)

    def units(ref, q, low, high):
        return jnp.concatenate([ref[q, u] for u in range(low, high)], axis=1)

    def exchange_term(q):
        @pl.when(mine)
        def _():
            row_own(q).wait()

        @pl.when(below)
        def _():
            row_came(q).wait_recv()
            row_all(q).start()

        @pl.when(last)
        def _():
            row_all(q).wait_recv()

        left = units(r.rows, q, 0, g.wu)
        for low in range(0, rows, g.group):
            high = min(low + g.group, rows)
            right = units(r.cols, q, low // LANE, up(high, LANE) // LANE)[:, :high - low]
            r.exch[:, low:high] += dot(left, right, ((0,), (0,)))

    def applied_term(q):
        right = units(r.cols, q, 0, g.units)
        for gg in range(g.size_y):
            r.applied[gg * g.j:(gg + 1) * g.j, :] += dot(r.mall[gg, q], right, ((1,), (0,)))

    def level(k, act):
        def one(i, carry):
            zz = z + jnp.where(i < nx, -k, k)

            @pl.when((zz >= 0) & (zz < nz))
            def _():
                act(zz * nx + lax.rem(x + lax.rem(i, nx), nx))

            return carry

        lax.fori_loop(0, 2 * nx if k else nx, one, 0)

    def arrive_x(k):
        for side in ((-1, 1) if k else (1,)):
            zz = z + side * k

            @pl.when((zz >= 0) & (zz < nz))
            def _(zz=zz):
                zz = jnp.clip(zz, 0, nz - 1)
                for sub in range(g.na):
                    for e in range(1, nx):
                        sideways(zz, sub, e, True).wait_recv()
                        pass_rows(zz * nx + lax.rem(x - e + nx, nx), sub)

        def own_rows(q):
            @pl.when(mine)
            def _():
                row_own(q).start()

        level(k, own_rows)

    def arrive_z(k, slot):
        for up_way in (True, False):
            zz = z - k if up_way else z + k

            @pl.when((zz >= 0) & (zz < nz))
            def _(zz=zz, up_way=up_way):
                zz = jnp.clip(zz, 0, nz - 1)
                sems = (r.send_u, r.recv_u) if up_way else (r.send_d, r.recv_d)
                ref = part_of(zz, slot)
                remote(ref, ref, sems[0].at[k - 1, slot], sems[1].at[k - 1, slot], partner).wait_recv()
                if k < nz - 1:
                    @pl.when((z < nz - 1) if up_way else (z > 0))
                    def _():
                        (upward if up_way else downward)(k, slot).start()
                if slot < g.na:
                    for e in range(1, nx):
                        sideways(zz, slot, e, False).start()
                    pass_rows(zz * nx + x, slot)
                else:
                    pass_rows(zz * nx + slot - g.na, g.na)

    def drain_first():
        for zz in range(nz):
            for e in range(1, nx):
                x_part(zz, e).wait_send()
        for d in range(1, nz):
            z_part(d).wait_send()
            block_z(d, False).wait_send()

        @pl.when(c == 0)
        def _():
            for d in range(nz):
                for e in range(1, nx):
                    block_x(gy, at(d, 0), d, e).wait_send()
                for e in range(nx):
                    for f in range(1, ny):
                        block_y(gy, at(d, e), d * nx + e, f).wait_send()

        @pl.when(c == 1)
        def _():
            for d in range(nz):
                for f in range(1, ny):
                    block_y(gy, at(d, 0), d, f).wait_send()
                for f in range(ny):
                    for e in range(1, nx):
                        block_x(group(f, c), at(d, 0), d * ny + f, e).wait_send()

        for d in range(nz):
            for e in range(nx):
                for f in range(ny):
                    block_c(d, e, f, c).wait_send()

    def drain_mixed():
        for d in range(1, g.size_y):
            mix_y(d).wait_send()
        for d in range(1, g.size_x):
            mix_x(d, False).wait_send()
        for f in range(1, ny):
            mix_share(f, False).wait_send()
        for f in range(ny):
            mix_core(f, c).wait_send()

        def hear(step, carry):
            stat_copy(lax.rem(me + step, devices), step, me).wait_recv()
            return carry

        lax.fori_loop(1, devices, hear, 0)

        def told(step, carry):
            stat_copy(me, step, me).wait_send()
            return carry

        lax.fori_loop(1, devices, told, 0)
        r.sland[me] = r.stats[...]
        r.sums[...] = jnp.sum(r.sland[...], axis=0)

    def drain_level(k):
        for slot in range(g.slots):
            @pl.when((z >= k) & (z < nz - 1))
            def _(slot=slot):
                upward(k, slot).wait_send()

            @pl.when((z + k < nz) & (z > 0))
            def _(slot=slot):
                downward(k, slot).wait_send()

    def drain_x(k):
        for e in range(1, nx):
            for side in ((-1, 1) if k else (1,)):
                zz = z + side * k

                @pl.when((zz >= 0) & (zz < nz))
                def _(zz=zz, e=e):
                    zz = jnp.clip(zz, 0, nz - 1)
                    for sub in range(g.na if k else g.na + 1):
                        sideways(zz, sub, e, False).wait_send()

    for k in range(1, nz):
        for slot in range(g.slots):
            arrive_z(k, slot)
            if slot == 1:
                if k == 1:
                    drain_first()
                else:
                    drain_level(k - 2)
                    drain_x(k - 2)
                if k == nz - 1:
                    drain_mixed()
            if slot == min(2, g.slots - 1):
                arrive_x(k - 1)
            if slot == g.slots - 2:
                if k == 2:
                    for f in range(ny):
                        if f > 0:
                            mix_share(f, True).wait_recv()
                            mix_core(f, c).start()
                    for f in range(ny):
                        mix_core(f, 1 - c).wait_recv()
                    level(0, applied_term)
                level(k - 1, exchange_term)
                if k >= 2:
                    level(k - 1, applied_term)
        if k == 1:
            for d in range(1, g.size_x):
                mix_x(d, True).wait_recv()
            for f in range(1, ny):
                mix_share(f, False).start()
            mix_core(0, c).start()
    arrive_x(nz - 1)
    drain_x(nz - 2)
    level(nz - 1, applied_term)

    low = r.applied[:, :rows].astype(BF16)

    def back_c(n, core):
        return remote(r.bpart.at[n, core], r.bland.at[n], r.send_v.at[n], r.recv_v.at[n], partner)

    def back_y(n, f):
        to = lax.rem(y + f, ny)
        return remote(r.bsum.at[n, to], r.byland.at[n, f], r.send_b.at[n, f], r.recv_b.at[n, f], (gx, to * 2 + c))

    for n in range(g.chunks):
        start, stop = n * g.step, min((n + 1) * g.step, g.depth)
        value = dot(low, r.projv[start:stop, :], ((1,), (1,)))
        for gg in range(g.size_y):
            r.bpart[n, gg % 2, gg // 2, :, :stop - start] = value[gg * g.j:(gg + 1) * g.j].astype(BF16)
        back_c(n, 1 - c).start()
    for n in range(g.chunks):
        back_c(n, 1 - c).wait_recv()
        total = r.bpart[n, c].astype(F32) + r.bland[n].astype(F32)
        r.bsum[n] = total.astype(BF16)
        for f in range(1, ny):
            back_y(n, f).start()
    level(nz - 1, exchange_term)
    for n in range(g.chunks):
        total = r.bpart[n, c, y].astype(F32) + r.bland[n, y].astype(F32)
        for f in range(1, ny):
            back_y(n, f).wait_recv()
            total = total + r.byland[n, f].astype(F32)
        start, stop = n * g.step, min((n + 1) * g.step, g.depth)
        r.back[:, start:stop] = total[:g.share, :stop - start]

    drain_level(nz - 2)
    drain_x(nz - 1)
    for n in range(g.chunks):
        back_c(n, 1 - c).wait_send()
        for f in range(1, ny):
            back_y(n, f).wait_send()

    def drain(q, carry):
        @pl.when(mine)
        def _():
            for f in range(1, ny):
                row_y_all(q, f).wait_send()
            row_c_all(q).wait_send()

        @pl.when(below)
        def _():
            row_all(q).wait_send()

        return carry

    lax.fori_loop(0, g.size_x, drain, 0)


def whole(g, orbitals, projector, integrals):
    dma, vmem = pltpu.SemaphoreType.DMA, pltpu.VMEM
    nz, nx, ny, occ = g.nz, g.nx, g.ny, g.occ
    devices = g.size_x * g.size_y
    scratch = dict(
        orbv=vmem(orbitals.shape, BF16),
        projv=vmem(projector.shape, BF16),
        integ=vmem((g.wide, g.total), BF16),
        part=vmem((nz, nx, g.rx, g.lz), BF16),
        xland=vmem((nx, nz, g.rx, g.lz), BF16),
        zsum=vmem((nz, g.rx, g.lz), BF16),
        zland=vmem((nz, g.rx, g.lz), BF16),
        agb=vmem((g.size_y, g.size_x, g.rx, g.lz), BF16),
        admm=vmem((occ, g.total), BF16),
        own=vmem((occ, g.own), BF16),
        cols=vmem((g.size_x, g.units, occ, LANE), BF16),
        rows=vmem((g.size_x, g.wu, occ, LANE), BF16),
        mixed=vmem((occ, occ), F32),
        trace=vmem((1, SUB * LANE), F32),
        mpart=vmem((g.size_y, g.j, occ), BF16),
        mland=vmem((g.size_y, g.j, occ), BF16),
        mall=vmem((g.size_y, g.size_x, g.j, occ), BF16),
        stats=vmem((1, LANE), F32),
        sland=vmem((devices, 1, LANE), F32),
        applied=vmem((g.size_y * g.j, g.wide), F32),
        bpart=vmem((g.chunks, 2, ny, g.j, g.step), BF16),
        bland=vmem((g.chunks, ny, g.j, g.step), BF16),
        bsum=vmem((g.chunks, ny, g.j, g.step), BF16),
        byland=vmem((g.chunks, ny, g.j, g.step), BF16),
        load_sem=dma((5,)),
        int_sem=dma((g.subs,)),
        row_sem=dma((g.size_x,)),
    )
    for letter, shape in dict(
        p=(nz, nx), q=(nz,), az=(nz,), ax=(nz * ny, nx), ay=(nz * nx, ny), ac=(nz * nx * ny,),
        u=(nz, g.slots), d=(nz, g.slots), x=(nz, g.subs, nx), m=(g.size_y,), n=(g.size_x,), o=(ny,), r=(ny,),
        s=(devices,), v=(g.chunks,), b=(g.chunks, ny),
    ).items():
        scratch["send_" + letter] = dma(shape)
        scratch["recv_" + letter] = dma(shape)
    scratch.update(
        send_y=dma((g.size_x, ny)), recv_y=dma((g.size_x,)), send_c=dma((g.size_x,)),
        recv_c=dma((g.size_x,)), send_w=dma((g.size_x,)),
    )
    names = ["orb_h", "proj_h", "int_h", "exch", "back", "sums"] + list(scratch)
    return pl.pallas_call(
        functools.partial(whole_kernel, g, names),
        out_shape=(
            vmem((g.window, g.rows), F32),
            vmem((g.share, g.depth), F32),
            vmem((1, LANE), F32),
        ),
        in_specs=[pl.BlockSpec(memory_space=pl.ANY)] * 3,
        out_specs=[pl.BlockSpec(memory_space=pltpu.VMEM)] * 3,
        scratch_shapes=list(scratch.values()),
        compiler_params=pltpu.CompilerParams(collective_id=1, has_side_effects=True, vmem_limit_bytes=LIMIT),
    )(orbitals, projector, integrals)


def finish_kernel(g, exch, back, sums, exch_o, back_o, energy, trace, sem, *spare):
    tall = up(-(-g.block // 8), 8)
    turn = lax.rem(lax.axis_index("gx"), g.per)
    begins = [i * g.block - g.firsts[i] for i in range(g.per)]
    skip, ready = 0, exch
    if spare:
        ready = spare[0]
        for i in range(g.per):
            @pl.when(turn == i)
            def _(i=i):
                ready[...] = exch[begins[i]:begins[i] + g.block, :]
    else:
        for i in range(g.per):
            skip = jnp.where(turn == i, begins[i] // 8, skip)
    copies = [pltpu.make_async_copy(back, back_o, sem.at[0])]
    for i, low in enumerate(range(0, g.block, tall)):
        high = min(low + tall, g.block)
        source = ready.at[low:high] if spare else ready.at[pl.ds(pl.multiple_of(skip * 8 + low, 8), high - low)]
        copies.append(pltpu.make_async_copy(source, exch_o.at[low:high], sem.at[i + 1]))
    for copy in copies:
        copy.start()
    lane = lax.broadcasted_iota(jnp.int32, (1, LANE), 1)
    value = sums[...]
    energy[...] = jnp.sum(jnp.where(lane == 0, value, 0.0), keepdims=True) * (-0.5 / (g.total * g.occ))
    trace[...] = jnp.sum(jnp.where(lane == 1, value, 0.0), keepdims=True) * (1.0 / g.total)
    for copy in copies:
        copy.wait()


def finish(g, exch, back, sums):
    vmem = pl.BlockSpec(memory_space=pltpu.VMEM)
    hbm = pl.BlockSpec(memory_space=pl.ANY)
    odd = any((i * g.block - g.firsts[i]) % 8 for i in range(g.per))
    spare = [pltpu.VMEM((g.block, g.rows), F32)] if odd else []
    return pl.pallas_call(
        functools.partial(finish_kernel, g),
        out_shape=(
            jax.ShapeDtypeStruct((g.block, g.rows), F32),
            jax.ShapeDtypeStruct(back.shape, F32),
            jax.ShapeDtypeStruct((1, 1), F32),
            jax.ShapeDtypeStruct((1, 1), F32),
        ),
        in_specs=[vmem] * 3,
        out_specs=[hbm, hbm, vmem, vmem],
        scratch_shapes=[pltpu.SemaphoreType.DMA((9,))] + spare,
        compiler_params=pltpu.CompilerParams(vmem_limit_bytes=2 * 1024 * 1024 + 2 * (exch.size + back.size) * 4),
    )(exch, back, sums)


def on_device(size_x, size_y, orbitals, projector, integrals):
    g = layout(size_x, size_y, projector.shape[0], projector.shape[1], orbitals.shape[1])
    exchange, back, energy, trace = finish(g, *whole(g, orbitals.T, projector.T, integrals))
    return (exchange, back.T, energy.reshape(()), trace.reshape(()))


def solution(mesh):
    return jax.shard_map(
        functools.partial(on_device, mesh.shape["gx"], mesh.shape["gy"]),
        mesh=mesh,
        in_specs=(P("gx", None), P("gy", "gx"), P("gx", "gy", None)),
        out_specs=(P("gx", "gy"), P("gx", "gy"), P(), P()),
        check_vma=False,
    )
```

```python
import functools
import types

import jax
import jax.numpy as jnp
from jax import lax
from jax.experimental import pallas as pl
from jax.experimental.pallas import tpu as pltpu
from jax.sharding import PartitionSpec as P

MESH = pl.DeviceIdType.MESH
LIMIT = 57 * 1024 * 1024
LANE = 128
SUB = 2
F32, BF16 = jnp.float32, jnp.bfloat16


def factor(size):
    inner = 1
    while inner * inner * 4 <= size:
        inner *= 2
    return size // inner, inner


def up(value, unit):
    return -(-value // unit) * unit


def remote(src, dst, send, recv, dev):
    return pltpu.make_async_remote_copy(
        src_ref=src, dst_ref=dst, send_sem=send, recv_sem=recv, device_id=dev, device_id_type=MESH
    )


def dot(a, b, dims):
    return lax.dot_general(a, b, (dims, ((), ())), preferred_element_type=F32)


def layout(size_x, size_y, rows, depth, occ):
    g = types.SimpleNamespace(size_x=size_x, size_y=size_y, rows=rows, depth=depth, occ=occ)
    g.nz, g.nx = factor(size_x)
    g.ny = size_y // 2
    g.total = rows * size_y
    g.lz = up(-(-rows // g.nz), LANE)
    g.waves = g.lz // LANE
    g.rx = up(-(-occ // g.nx), 8)
    g.off = [min(i * g.rx, occ - g.rx) for i in range(g.nx)]
    g.wide = up(rows, SUB * LANE)
    g.own = max(g.wide, g.nz * g.lz)
    g.units = g.wide // LANE
    g.subs = g.units // SUB
    g.na = g.subs - 1
    g.slots = g.na + g.nx
    g.block = g.total // size_x
    g.per = size_x // size_y
    g.window = max(up(i * g.block % LANE + g.block, LANE) for i in range(g.per))
    g.wu = g.window // LANE
    g.firsts = [min(i * g.block // LANE * LANE, g.wide - g.window) for i in range(g.per)]
    g.begins = [i * g.block - g.firsts[i] for i in range(g.per)]
    g.odd = any(begin % 8 for begin in g.begins)
    g.share = occ // size_y
    g.j = up(g.share, 8)
    g.step = 512
    g.chunks = -(-depth // g.step)
    g.group = 512 if g.wide % 512 == 0 else 256
    return g


def flip(value, mask, size):
    if size & (size - 1):
        return lax.rem(value + mask, size)
    bit = 1
    while bit < size:
        if mask & bit:
            value = value + bit - 2 * bit * lax.rem(value // bit, 2)
        bit *= 2
    return value


def unflip(value, mask, size):
    return lax.rem(value - mask + size, size) if size & (size - 1) else flip(value, mask, size)


def greet(size_x, size_y):
    gx, gy = lax.axis_index("gx"), lax.axis_index("gy")
    barrier = pltpu.get_barrier_semaphore()

    def hello(step, carry):
        other = lax.rem(gx * size_y + gy + step, size_x * size_y)
        pl.semaphore_signal(
            barrier, inc=1, device_id=(other // size_y, lax.rem(other, size_y)), device_id_type=MESH
        )
        return carry

    lax.fori_loop(1, size_x * size_y, hello, 0)
    pl.semaphore_wait(barrier, size_x * size_y - 1)


def whole_kernel(g, names, *refs):
    r = types.SimpleNamespace(**dict(zip(names, refs)))
    nz, nx, ny, occ, rows = g.nz, g.nx, g.ny, g.occ, g.rows
    gx, gy = lax.axis_index("gx"), lax.axis_index("gy")
    z, x = gx // nx, lax.rem(gx, nx)
    y, c = gy // 2, lax.rem(gy, 2)
    partner = (gx, gy + 1 - 2 * c)

    def left(ref, sem):
        remote(ref, ref, sem, r.spare, partner).wait_send()

    loads = [pltpu.make_async_copy(r.orb_h, r.orbv, r.load_sem.at[0])]
    pieces = r.load_sem.shape[0] - 1
    tall = up(-(-g.depth // pieces), 8)
    for i in range(pieces):
        low, high = i * tall, min((i + 1) * tall, g.depth)
        loads.append(pltpu.make_async_copy(r.proj_h.at[low:high], r.projv.at[low:high], r.load_sem.at[i + 1]))
    for load in loads:
        load.start()
    span = SUB * LANE

    def int_load(s):
        low, high = s * span, min((s + 1) * span, rows)
        return pltpu.make_async_copy(r.int_h.at[0, low:high], r.integ.at[low:high], r.int_sem.at[s])

    greet(g.size_x, g.size_y)
    for load in loads:
        load.wait()
    for s in range(g.subs):
        int_load(s).start()

    def x_part(zz, w, e):
        to = lax.rem(x + e, nx)
        return remote(
            r.part.at[zz, w, to], r.xland.at[e - 1, zz, w], r.send_p, r.recv_p.at[zz, w, e - 1], (z * nx + to, gy)
        )

    tail = (rows - 1) // g.lz

    def put(zz, value):
        for w in range(g.waves):
            seg = value[:, w * LANE:(w + 1) * LANE].astype(BF16)
            if seg.shape[1]:
                for xx in range(nx):
                    r.part[zz, w, xx, :, :seg.shape[1]] = seg[g.off[xx]:g.off[xx] + g.rx]

    for d in reversed(range(nz)):
        zz = flip(z, d, nz)

        @pl.when(zz < tail)
        def _(zz=zz):
            put(zz, dot(r.orbv[...], r.projv[:, pl.ds(pl.multiple_of(zz * g.lz, LANE), g.lz)], ((1,), (0,))))

        @pl.when(zz == tail)
        def _():
            put(tail, dot(r.orbv[...], r.projv[:, tail * g.lz:rows], ((1,), (0,))))

        for w in range(g.waves):
            for e in range(1, nx):
                x_part(zz, w, e).start()

    def x_sum(zz, w):
        value = r.part[zz, w, x].astype(F32)
        for e in range(1, nx):
            x_part(zz, w, e).wait_recv()
            value = value + r.xland[e - 1, zz, w].astype(F32)
        return value

    def z_part(d, w):
        return remote(
            r.zsum.at[d - 1, w], r.zland.at[d - 1, w], r.send_q, r.recv_q.at[d - 1, w], (flip(z, d, nz) * nx + x, gy)
        )

    for d in reversed(range(1, nz)):
        for w in range(g.waves):
            r.zsum[d - 1, w] = x_sum(flip(z, d, nz), w).astype(BF16)
            z_part(d, w).start()

    def at(d, e):
        return unflip(z, d, nz) * nx + lax.rem(x - e + nx, nx)

    def group(f, core):
        return lax.rem(y - f + ny, ny) * 2 + core

    def block_up(k, w):
        ref = r.agb.at[gy, w, jnp.maximum(z - k, 0) * nx + x]
        return remote(ref, ref, r.send_au.at[k], r.recv_au.at[k, w], (jnp.minimum(z + 1, nz - 1) * nx + x, gy))

    def block_down(k, w):
        ref = r.agb.at[gy, w, jnp.minimum(z + k, nz - 1) * nx + x]
        return remote(ref, ref, r.send_ad.at[k], r.recv_ad.at[k, w], (jnp.maximum(z - 1, 0) * nx + x, gy))

    def block_came(zz, k, w, rising):
        ref = r.agb.at[gy, w, zz * nx + x]
        sem = r.recv_au if rising else r.recv_ad
        return remote(ref, ref, r.spare, sem.at[k - 1, w], partner)

    def block_x(gg, w, q, slot, e):
        ref = r.agb.at[gg, w, q]
        return remote(
            ref, ref, r.send_ax, r.recv_ax.at[slot, w, e - 1], (z * nx + lax.rem(x + e, nx), gy)
        )

    def block_y(gg, w, q, slot, f):
        ref = r.agb.at[gg, w, q]
        return remote(
            ref, ref, r.send_ay, r.recv_ay.at[slot, w, f - 1], (gx, lax.rem(y + f, ny) * 2 + c)
        )

    def block_c(f, w, core):
        ref = r.agb.at[group(f, core), w]
        return remote(ref, ref, r.send_ac, r.recv_ac.at[f, w], partner)

    for w in range(g.waves):
        total = x_sum(z, w)
        for d in range(1, nz):
            z_part(d, w).wait_recv()
            total = total + r.zland[d - 1, w].astype(F32)
        r.agb[gy, w, gx] = total.astype(BF16)

        @pl.when(z < nz - 1)
        def _(w=w):
            block_up(0, w).start()

        @pl.when(z > 0)
        def _(w=w):
            block_down(0, w).start()

        for e in range(1, nx):
            block_x(gy, w, gx, jnp.where(c == 0, z, z * ny), e).start()
        for f in range(1, ny):
            block_y(gy, w, gx, jnp.where(c == 0, z * nx, z), f).start()

    def planes(k, act):
        for rising in ((True, False) if k else (True,)):
            zz = z - k if rising else z + k

            @pl.when((zz >= 0) & (zz < nz))
            def _(zz=zz, rising=rising):
                act(jnp.clip(zz, 0, nz - 1), rising)

    def first_stage(k, x_first):
        def act(zz, rising):
            for w in range(g.waves):
                block_came(zz, k, w, rising).wait_recv()
                if k < nz - 1:
                    @pl.when((z < nz - 1) if rising else (z > 0))
                    def _():
                        (block_up if rising else block_down)(k, w).start()
                for e in range(1, nx):
                    block_x(gy, w, zz * nx + x, zz if x_first else zz * ny, e).start()
                for f in range(1, ny):
                    block_y(gy, w, zz * nx + x, zz * nx if x_first else zz, f).start()

        planes(k, act)

    def second_stage(k, x_first):
        def act(zz, rising):
            for w in range(g.waves):
                if x_first:
                    for e in range(1, nx):
                        q = zz * nx + lax.rem(x - e + nx, nx)
                        block_x(gy, w, q, zz, e).wait_recv()
                        for f in range(1, ny):
                            block_y(gy, w, q, zz * nx + e, f).start()
                else:
                    for f in range(1, ny):
                        block_y(group(f, c), w, zz * nx + x, zz, f).wait_recv()
                        for e in range(1, nx):
                            block_x(group(f, c), w, zz * nx + x, zz * ny + f, e).start()

        planes(k, act)

    def third_stage(w, x_first):
        for f in range(1 if x_first else 0, ny):
            for d in range(nz):
                zz = flip(z, d, nz)
                if x_first:
                    for e in range(nx):
                        q = zz * nx + lax.rem(x - e + nx, nx)
                        block_y(group(f, c), w, q, zz * nx + e, f).wait_recv()
                else:
                    for e in range(1, nx):
                        q = zz * nx + lax.rem(x - e + nx, nx)
                        block_x(group(f, c), w, q, zz * ny + f, e).wait_recv()
            block_c(f, w, c).start()

    for x_first in (True, False):
        @pl.when(c == (0 if x_first else 1))
        def _(x_first=x_first):
            for k in range(1, nz):
                first_stage(k, x_first)
                second_stage(k - 1, x_first)
            second_stage(nz - 1, x_first)
            for w in range(g.waves):
                if x_first:
                    block_c(0, w, c).start()
                third_stage(w, x_first)

    for w in range(g.waves):
        for f in range(ny):
            block_c(f, w, 1 - c).wait_recv()

    lane = lax.broadcasted_iota(jnp.int32, (g.rx, g.lz), 1)

    def joined(gg, q):
        return jnp.concatenate([r.agb[gg, w, q] for w in range(g.waves)], axis=1)

    for gg in range(g.size_y):
        for zz in range(nz):
            width = min(g.lz, rows - zz * g.lz)
            if width <= 0:
                continue
            base = gg * rows + zz * g.lz
            for xx in range(nx):
                r.admm[g.off[xx]:g.off[xx] + g.rx, base:base + width] = joined(gg, zz * nx + xx)[:, :width]
    for zz in range(nz):
        for xx in range(nx):
            piece = joined(gy, zz * nx + xx)
            piece = jnp.where(lane + zz * g.lz < rows, piece.astype(F32), 0.0).astype(BF16)
            r.own[g.off[xx]:g.off[xx] + g.rx, zz * g.lz:(zz + 1) * g.lz] = piece

    devices = g.size_x * g.size_y
    me = gx * g.size_y + gy
    root = gx // g.per
    root_y, root_c = root // 2, lax.rem(root, 2)
    turn = lax.rem(gx, g.per)
    first = 0
    for i in range(g.per):
        first = jnp.where(turn == i, g.firsts[i] // LANE, first)
    mine = gy == root
    below = (y != root_y) & (c == root_c)
    last = c != root_c

    def part_of(zz, slot):
        if slot < g.na:
            return r.cols.at[zz * nx + x, pl.ds(SUB * slot, SUB)]
        return r.cols.at[zz * nx + slot - g.na, pl.ds(SUB * g.na, SUB)]

    def upward(k, slot):
        ref = part_of(jnp.maximum(z - k, 0), slot)
        return remote(ref, ref, r.send_u.at[k], r.recv_u.at[k, slot], (jnp.minimum(z + 1, nz - 1) * nx + x, gy))

    def downward(k, slot):
        ref = part_of(jnp.minimum(z + k, nz - 1), slot)
        return remote(ref, ref, r.send_d.at[k], r.recv_d.at[k, slot], (jnp.maximum(z - 1, 0) * nx + x, gy))

    def sideways(zz, sub, e, came):
        ref = r.cols.at[zz * nx + (lax.rem(x - e + nx, nx) if came else x), pl.ds(SUB * sub, SUB)]
        return remote(
            ref, ref, r.send_x.at[zz], r.recv_x.at[zz, sub, e - 1], (z * nx + lax.rem(x + e, nx), gy)
        )

    def row_y(q, unit, f):
        spot = unit - first
        return remote(
            r.cols.at[q, unit], r.rows.at[q, spot], r.send_y.at[f - 1], r.recv_y.at[q], (gx, lax.rem(y + f, ny) * 2 + c)
        )

    def row_c(q, unit):
        spot = unit - first
        return remote(r.cols.at[q, unit], r.rows.at[q, spot], r.send_c, r.recv_c.at[q], partner)

    def row_all(q):
        return remote(r.rows.at[q], r.rows.at[q], r.send_w, r.recv_c.at[q], partner)

    def row_came(q):
        return remote(r.rows.at[q], r.rows.at[q], r.spare, r.recv_y.at[q], partner)

    def row_own(q):
        return pltpu.make_async_copy(r.cols.at[q, pl.ds(first, g.wu)], r.rows.at[q], r.row_sem.at[q])

    def pass_rows(q, sub):
        for h in range(SUB):
            unit = sub * SUB + h

            @pl.when(mine & (unit >= first) & (unit < first + g.wu))
            def _():
                for f in range(1, ny):
                    row_y(q, unit, f).start()
                row_c(q, unit).start()

    r.mixed[...] = jnp.zeros_like(r.mixed)
    r.trace[...] = jnp.zeros_like(r.trace)
    for s in range(g.subs):
        int_load(s).wait()
    spots = lax.broadcasted_iota(jnp.int32, (occ, span), 1)

    def half(i, carry):
        s = lax.rem(i + g.na, g.subs)
        start = pl.multiple_of(s * span, span)
        value = dot(r.admm[...], r.integ[pl.ds(start, span), :], ((1,), (1,)))
        value = jnp.where(spots + start < rows, value, 0.0)
        low = value.astype(BF16)
        for h in range(SUB):
            r.cols[gx, SUB * s + h] = low[:, h * LANE:(h + 1) * LANE]

        @pl.when(i == 0)
        def _():
            for e in range(1, nx):
                sideways(z, g.na, e, False).start()

        @pl.when(i > 0)
        def _():
            ref = r.cols.at[gx, pl.ds(SUB * s, SUB)]

            @pl.when(z < nz - 1)
            def _():
                remote(ref, ref, r.send_u.at[0], r.recv_u.at[0, s], (jnp.minimum(z + 1, nz - 1) * nx + x, gy)).start()

            @pl.when(z > 0)
            def _():
                remote(ref, ref, r.send_d.at[0], r.recv_d.at[0, s], (jnp.maximum(z - 1, 0) * nx + x, gy)).start()

            for e in range(1, nx):
                sideways(z, s, e, False).start()

        for h in range(SUB):
            unit = SUB * s + h

            @pl.when(mine & (unit >= first) & (unit < first + g.wu))
            def _():
                for f in range(1, ny):
                    row_y(gx, unit, f).start()
                row_c(gx, unit).start()

        exact = low.astype(F32)
        r.trace[...] += jnp.sum(exact * exact, axis=0, keepdims=True)
        r.mixed[...] += dot(r.own[:, pl.ds(start, span)], low, ((1,), (1,)))
        return carry

    lax.fori_loop(0, g.subs, half, 0)

    def z_send(k, slot):
        @pl.when((z >= k) & (z < nz - 1))
        def _():
            upward(k, slot).start()

        @pl.when((z + k < nz) & (z > 0))
        def _():
            downward(k, slot).start()

    for e in range(nx):
        for xx in range(nx):
            @pl.when(lax.rem(x - e + nx, nx) == xx)
            def _(e=e, xx=xx):
                if e > 0:
                    sideways(z, g.na, e, True).wait_recv()
                    pass_rows(z * nx + xx, g.na)
                z_send(0, g.na + xx)

    low = r.mixed[...].astype(BF16)
    row_i = lax.broadcasted_iota(jnp.int32, (g.j, occ), 0)
    col_i = lax.broadcasted_iota(jnp.int32, (g.j, occ), 1)
    for gg in range(g.size_y):
        pick = ((row_i < g.share) & (col_i == row_i + gg * g.share)).astype(F32).astype(BF16)
        r.mpart[gg] = dot(pick, low, ((1,), (0,))).astype(BF16)

    def mix_y(d):
        to = lax.rem(gy + d, g.size_y)
        return remote(r.mpart.at[to], r.mland.at[d - 1], r.send_m, r.recv_m.at[d - 1], (gx, to))

    for d in range(1, g.size_y):
        mix_y(d).start()
    total = r.mpart[gy].astype(F32)
    for d in range(1, g.size_y):
        mix_y(d).wait_recv()
        total = total + r.mland[d - 1].astype(F32)
    r.mall[gy, gx] = total.astype(BF16)

    def mix_z(d, came):
        ref = r.mall.at[gy, at(d, 0) if came else gx]
        return remote(ref, ref, r.send_n, r.recv_n.at[d - 1], (flip(z, d, nz) * nx + x, gy))

    def mix_x(d, e, came):
        ref = r.mall.at[gy, at(d, e if came else 0)]
        return remote(ref, ref, r.send_k, r.recv_k.at[d, e - 1], (z * nx + lax.rem(x + e, nx), gy))

    def mix_share(f, came):
        ref = r.mall.at[group(f, c) if came else gy]
        return remote(ref, ref, r.send_o, r.recv_o.at[f - 1], (gx, lax.rem(y + f, ny) * 2 + c))

    def mix_core(f, core):
        ref = r.mall.at[group(f, core)]
        return remote(ref, ref, r.send_r, r.recv_r.at[f], partner)

    for d in range(1, nz):
        mix_z(d, False).start()
    for e in range(1, nx):
        mix_x(0, e, False).start()
    stat_lane = lax.broadcasted_iota(jnp.int32, (1, LANE), 1)
    energy_part, trace_part = jnp.sum(total * total), jnp.sum(r.trace[...])
    r.stats[...] = jnp.where(stat_lane == 0, energy_part, jnp.where(stat_lane == 1, trace_part, 0.0))

    def stat_copy(to):
        return remote(r.stats, r.sland.at[me], r.send_s, r.recv_s, (to // g.size_y, lax.rem(to, g.size_y)))

    def tell(step, carry):
        stat_copy(lax.rem(me + step, devices)).start()
        return carry

    lax.fori_loop(1, devices, tell, 0)

    r.acc[...] = jnp.zeros_like(r.acc)
    r.applied[...] = jnp.zeros_like(r.applied)

    def units(ref, q, low, high):
        return jnp.concatenate([ref[q, u] for u in range(low, high)], axis=1)

    def exchange_term(zz):
        for xx in range(nx):
            q = zz * nx + xx

            @pl.when(mine)
            def _(q=q):
                row_own(q).wait()

            @pl.when(below)
            def _(q=q):
                row_came(q).wait_recv()
                row_all(q).start()

        @pl.when(last)
        def _():
            for xx in range(nx):
                row_all(zz * nx + xx).wait_recv()

        lefts = [units(r.rows, zz * nx + xx, 0, g.wu) for xx in range(nx)]
        for low in range(0, rows, g.group):
            high = min(low + g.group, rows)
            value = r.acc[:, low:high]
            for xx in range(nx):
                right = units(r.cols, zz * nx + xx, low // LANE, up(high, LANE) // LANE)[:, :high - low]
                value = value + dot(lefts[xx], right, ((0,), (0,)))
            r.acc[:, low:high] = value

    def applied_term(zz):
        value = r.applied[...]
        for xx in range(nx):
            q = zz * nx + xx
            left = jnp.concatenate([r.mall[gg, q] for gg in range(g.size_y)], axis=0)
            value = value + dot(left, units(r.cols, q, 0, g.units), ((1,), (0,)))
        r.applied[...] = value

    def level(k, act):
        def one(i, carry):
            zz = z - k + 2 * k * i

            @pl.when((zz >= 0) & (zz < nz))
            def _():
                act(zz)

            return carry

        lax.fori_loop(0, 2 if k else 1, one, 0)

    def arrive_x(k):
        for side in ((-1, 1) if k else (1,)):
            zz = z + side * k

            @pl.when((zz >= 0) & (zz < nz))
            def _(zz=zz):
                zz = jnp.clip(zz, 0, nz - 1)
                for sub in range(g.na):
                    for e in range(1, nx):
                        sideways(zz, sub, e, True).wait_recv()
                        pass_rows(zz * nx + lax.rem(x - e + nx, nx), sub)

        def own_rows(zz):
            @pl.when(mine)
            def _():
                for xx in range(nx):
                    row_own(zz * nx + xx).start()

        level(k, own_rows)

    def arrive_z(k, slot):
        for up_way in (True, False):
            zz = z - k if up_way else z + k

            @pl.when((zz >= 0) & (zz < nz))
            def _(zz=zz, up_way=up_way):
                zz = jnp.clip(zz, 0, nz - 1)
                sem = r.recv_u if up_way else r.recv_d
                ref = part_of(zz, slot)
                remote(ref, ref, r.spare, sem.at[k - 1, slot], partner).wait_recv()
                if k < nz - 1:
                    @pl.when((z < nz - 1) if up_way else (z > 0))
                    def _():
                        (upward if up_way else downward)(k, slot).start()
                if slot < g.na:
                    for e in range(1, nx):
                        sideways(zz, slot, e, False).start()
                    pass_rows(zz * nx + x, slot)
                else:
                    pass_rows(zz * nx + slot - g.na, g.na)

    def drain_first():
        left(r.xland, r.send_p)
        left(r.zland, r.send_q)
        for k in range(nz - 1):
            @pl.when((z >= k) & (z < nz - 1))
            def _(k=k):
                left(r.agb.at[0, :, 0], r.send_au.at[k])

            @pl.when((z + k < nz) & (z > 0))
            def _(k=k):
                left(r.agb.at[0, :, 0], r.send_ad.at[k])

        left(r.agb.at[0:ny], r.send_ac)

        @pl.when(c == 0)
        def _():
            left(r.agb.at[0, :, 0:nz * (nx - 1)], r.send_ax)
            left(r.agb.at[0:ny - 1], r.send_ay)

        @pl.when(c == 1)
        def _():
            left(r.agb.at[0:ny * (nx - 1) // nx], r.send_ax)
            left(r.agb.at[0, :, 0:nz * (ny - 1)], r.send_ay)

    def drain_mixed():
        left(r.mland, r.send_m)
        left(r.mall.at[0, 0:nz - 1], r.send_n)
        left(r.mall.at[0, 0:nz * (nx - 1)], r.send_k)
        left(r.mall.at[0:ny - 1], r.send_o)
        left(r.mall.at[0:ny], r.send_r)
        others = r.sland.at[0:devices - 1]
        remote(others, others, r.send_s, r.recv_s, partner).wait()
        r.sland[me] = r.stats[...]
        r.sums[...] = jnp.sum(r.sland[...], axis=0)

    def drain_level(k):
        span_of = r.cols.at[0:SUB, 0:g.slots]

        @pl.when((z >= k) & (z < nz - 1))
        def _():
            left(span_of, r.send_u.at[k])

        @pl.when((z + k < nz) & (z > 0))
        def _():
            left(span_of, r.send_d.at[k])

    def drain_x(k):
        def act(zz, rising):
            left(r.cols.at[0:nx - 1, 0:SUB * (g.na if k else g.subs)], r.send_x.at[zz])

        planes(k, act)

    edge = (z == 0) | (z == nz - 1)

    def share_mixed():
        for d in range(nz):
            for e in range(1, nx):
                mix_x(d, e, True).wait_recv()
        for f in range(1, ny):
            mix_share(f, False).start()
        mix_core(0, c).start()

    def work(k):
        level(k - 1, exchange_term)
        if k == nz - 1:
            for f in range(ny):
                mix_core(f, 1 - c).wait_recv()
            for j in range(nz - 1):
                level(j, applied_term)

    for k in range(1, nz):
        for slot in range(g.slots):
            arrive_z(k, slot)
            if slot == 1:
                if k == 1:
                    drain_first()
                else:
                    drain_level(k - 2)
                    drain_x(k - 2)
            if slot == min(2, g.slots - 1):
                @pl.when(edge)
                def _(k=k):
                    arrive_x(k - 1)
            if slot == g.slots - 2:
                if k == 1:
                    for d in range(1, nz):
                        mix_z(d, True).wait_recv()
                        for e in range(1, nx):
                            mix_x(d, e, False).start()
                if k == nz - 1:
                    for f in range(1, ny):
                        mix_share(f, True).wait_recv()
                        mix_core(f, c).start()

                @pl.when(edge)
                def _(k=k):
                    work(k)

        @pl.when(jnp.logical_not(edge))
        def _(k=k):
            arrive_x(k - 1)
            if k == nz - 2:
                share_mixed()
            work(k)

        if k == nz - 2:
            @pl.when(edge)
            def _():
                share_mixed()
    drain_mixed()
    arrive_x(nz - 1)
    drain_x(nz - 2)
    level(nz - 1, applied_term)

    low = r.applied[:, :rows].astype(BF16)

    def back_c(n, core):
        return remote(r.bpart.at[n, core], r.bland.at[n], r.send_v, r.recv_v.at[n], partner)

    def back_y(n, f):
        to = lax.rem(y + f, ny)
        return remote(r.bsum.at[n, to], r.byland.at[n, f - 1], r.send_b, r.recv_b.at[n, f - 1], (gx, to * 2 + c))

    def back_on(n):
        back_c(n, 1 - c).wait_recv()
        total = r.bpart[n, c].astype(F32) + r.bland[n].astype(F32)
        r.bsum[n] = total.astype(BF16)
        for f in range(1, ny):
            back_y(n, f).start()

    for n in range(g.chunks):
        start, stop = n * g.step, min((n + 1) * g.step, g.depth)
        value = dot(low, r.projv[start:stop, :], ((1,), (1,)))
        for gg in range(g.size_y):
            r.bpart[n, gg % 2, gg // 2, :, :stop - start] = value[gg * g.j:(gg + 1) * g.j].astype(BF16)
        back_c(n, 1 - c).start()
        if n > 0:
            back_on(n - 1)
    back_on(g.chunks - 1)
    level(nz - 1, exchange_term)
    if g.odd:
        result = pltpu.make_async_copy(r.acc, r.exch, r.out_sem)
    else:
        skip = 0
        for i in range(g.per):
            skip = jnp.where(turn == i, g.begins[i] // 8, skip)
        result = pltpu.make_async_copy(
            r.acc.at[pl.ds(pl.multiple_of(skip * 8, 8), g.block)], r.exch, r.out_sem
        )
    result.start()
    for n in range(g.chunks):
        total = r.bpart[n, c, y].astype(F32) + r.bland[n, y].astype(F32)
        for f in range(1, ny):
            back_y(n, f).wait_recv()
            total = total + r.byland[n, f - 1].astype(F32)
        start, stop = n * g.step, min((n + 1) * g.step, g.depth)
        r.back[:, start:stop] = total[:g.share, :stop - start]

    drain_level(nz - 2)
    drain_x(nz - 1)
    left(r.bland, r.send_v)
    left(r.byland, r.send_b)

    @pl.when(mine)
    def _():
        for f in range(1, ny):
            left(r.rows, r.send_y.at[f - 1])
        left(r.rows, r.send_c)

    @pl.when(below)
    def _():
        left(r.rows, r.send_w)

    result.wait()


def whole(g, orbitals, projector, integrals):
    dma, vmem = pltpu.SemaphoreType.DMA, pltpu.VMEM
    nz, nx, ny, occ = g.nz, g.nx, g.ny, g.occ
    devices = g.size_x * g.size_y
    scratch = dict(
        orbv=vmem(orbitals.shape, BF16),
        projv=vmem(projector.shape, BF16),
        integ=vmem((g.wide, g.total), BF16),
        part=vmem((nz, g.waves, nx, g.rx, LANE), BF16),
        xland=vmem((nx - 1, nz, g.waves, g.rx, LANE), BF16),
        zsum=vmem((nz - 1, g.waves, g.rx, LANE), BF16),
        zland=vmem((nz - 1, g.waves, g.rx, LANE), BF16),
        agb=vmem((g.size_y, g.waves, g.size_x, g.rx, LANE), BF16),
        admm=vmem((occ, g.total), BF16),
        own=vmem((occ, g.own), BF16),
        cols=vmem((g.size_x, g.units, occ, LANE), BF16),
        rows=vmem((g.size_x, g.wu, occ, LANE), BF16),
        acc=vmem((g.window, g.rows), F32),
        mixed=vmem((occ, occ), F32),
        out_sem=dma(()),
        trace=vmem((1, SUB * LANE), F32),
        mpart=vmem((g.size_y, g.j, occ), BF16),
        mland=vmem((g.size_y - 1, g.j, occ), BF16),
        mall=vmem((g.size_y, g.size_x, g.j, occ), BF16),
        stats=vmem((1, LANE), F32),
        sland=vmem((devices, 1, LANE), F32),
        applied=vmem((g.size_y * g.j, g.wide), F32),
        bpart=vmem((g.chunks, 2, ny, g.j, g.step), BF16),
        bland=vmem((g.chunks, ny, g.j, g.step), BF16),
        bsum=vmem((g.chunks, ny, g.j, g.step), BF16),
        byland=vmem((g.chunks, ny - 1, g.j, g.step), BF16),
        load_sem=dma((5,)),
        int_sem=dma((g.subs,)),
        row_sem=dma((g.size_x,)),
    )
    one = ()
    for letter, sends, arrivals in (
        ("p", one, (nz, g.waves, nx - 1)),
        ("q", one, (nz - 1, g.waves)),
        ("au", (nz - 1,), (nz - 1, g.waves)),
        ("ad", (nz - 1,), (nz - 1, g.waves)),
        ("ax", one, (nz * ny, g.waves, nx - 1)),
        ("ay", one, (nz * nx, g.waves, ny - 1)),
        ("ac", one, (ny, g.waves)),
        ("u", (nz - 1,), (nz - 1, g.slots)),
        ("d", (nz - 1,), (nz - 1, g.slots)),
        ("x", (nz,), (nz, g.subs, nx - 1)),
        ("m", one, (g.size_y - 1,)),
        ("n", one, (nz - 1,)),
        ("k", one, (nz, nx - 1)),
        ("o", one, (ny - 1,)),
        ("r", one, (ny,)),
        ("s", one, one),
        ("v", one, (g.chunks,)),
        ("b", one, (g.chunks, ny - 1)),
        ("y", (ny - 1,), (g.size_x,)),
        ("c", one, (g.size_x,)),
    ):
        scratch["send_" + letter] = dma(sends)
        scratch["recv_" + letter] = dma(arrivals)
    scratch.update(send_w=dma(one), spare=dma(one))
    names = ["orb_h", "proj_h", "int_h", "exch", "back", "sums"] + list(scratch)
    return pl.pallas_call(
        functools.partial(whole_kernel, g, names),
        out_shape=(
            vmem((g.window if g.odd else g.block, g.rows), F32),
            vmem((g.share, g.depth), F32),
            vmem((1, LANE), F32),
        ),
        in_specs=[pl.BlockSpec(memory_space=pl.ANY)] * 3,
        out_specs=[pl.BlockSpec(memory_space=pl.ANY)] + [pl.BlockSpec(memory_space=pltpu.VMEM)] * 2,
        scratch_shapes=list(scratch.values()),
        compiler_params=pltpu.CompilerParams(collective_id=1, has_side_effects=True, vmem_limit_bytes=LIMIT),
    )(orbitals, projector, integrals)


def finish_kernel(g, exch, back, sums, exch_o, back_o, energy, trace, sem, *spare):
    tall = up(-(-g.block // 8), 8)
    ready = exch
    if spare:
        ready = spare[0]
        turn = lax.rem(lax.axis_index("gx"), g.per)
        for i in range(g.per):
            @pl.when(turn == i)
            def _(i=i):
                ready[...] = exch[g.begins[i]:g.begins[i] + g.block, :]
    copies = [pltpu.make_async_copy(back, back_o, sem.at[0])]
    for i, low in enumerate(range(0, g.block, tall)):
        high = min(low + tall, g.block)
        copies.append(pltpu.make_async_copy(ready.at[low:high], exch_o.at[low:high], sem.at[i + 1]))
    for copy in copies:
        copy.start()
    lane = lax.broadcasted_iota(jnp.int32, (1, LANE), 1)
    value = sums[...]
    energy[...] = jnp.sum(jnp.where(lane == 0, value, 0.0), keepdims=True) * (-0.5 / (g.total * g.occ))
    trace[...] = jnp.sum(jnp.where(lane == 1, value, 0.0), keepdims=True) * (1.0 / g.total)
    for copy in copies:
        copy.wait()


def finish(g, exch, back, sums):
    vmem = pl.BlockSpec(memory_space=pltpu.VMEM)
    hbm = pl.BlockSpec(memory_space=pl.ANY)
    spare = [pltpu.VMEM((g.block, g.rows), F32)] if g.odd else []
    return pl.pallas_call(
        functools.partial(finish_kernel, g),
        out_shape=(
            jax.ShapeDtypeStruct((g.block, g.rows), F32),
            jax.ShapeDtypeStruct(back.shape, F32),
            jax.ShapeDtypeStruct((1, 1), F32),
            jax.ShapeDtypeStruct((1, 1), F32),
        ),
        in_specs=[vmem] * 3,
        out_specs=[hbm, hbm, vmem, vmem],
        scratch_shapes=[pltpu.SemaphoreType.DMA((9,))] + spare,
        compiler_params=pltpu.CompilerParams(vmem_limit_bytes=2 * 1024 * 1024 + 2 * (exch.size + back.size) * 4),
    )(exch, back, sums)


def on_device(size_x, size_y, orbitals, projector, integrals):
    g = layout(size_x, size_y, projector.shape[0], projector.shape[1], orbitals.shape[1])
    exchange, back, energy, trace = finish(g, *whole(g, orbitals.T, projector.T, integrals))
    return (exchange, back.T, energy.reshape(()), trace.reshape(()))


def solution(mesh):
    return jax.shard_map(
        functools.partial(on_device, mesh.shape["gx"], mesh.shape["gy"]),
        mesh=mesh,
        in_specs=(P("gx", None), P("gy", "gx"), P("gx", "gy", None)),
        out_specs=(P("gx", "gy"), P("gx", "gy"), P(), P()),
        check_vma=False,
    )
```

```python
import functools
import types

import jax
import jax.numpy as jnp
from jax import lax
from jax.experimental import pallas as pl
from jax.experimental.pallas import tpu as pltpu
from jax.sharding import PartitionSpec as P

MESH = pl.DeviceIdType.MESH
LIMIT = 57 * 1024 * 1024
LANE = 128
SUB = 2
F32, BF16 = jnp.float32, jnp.bfloat16


def factor(size):
    inner = 1
    while inner * inner * 4 <= size:
        inner *= 2
    return size // inner, inner


def up(value, unit):
    return -(-value // unit) * unit


def remote(src, dst, send, recv, dev):
    return pltpu.make_async_remote_copy(
        src_ref=src, dst_ref=dst, send_sem=send, recv_sem=recv, device_id=dev, device_id_type=MESH
    )


def dot(a, b, dims):
    return lax.dot_general(a, b, (dims, ((), ())), preferred_element_type=F32)


def layout(size_x, size_y, rows, depth, occ):
    g = types.SimpleNamespace(size_x=size_x, size_y=size_y, rows=rows, depth=depth, occ=occ)
    g.nz, g.nx = factor(size_x)
    g.ny = size_y // 2
    g.total = rows * size_y
    g.lz = up(-(-rows // g.nz), LANE)
    g.waves = g.lz // LANE
    g.rx = up(-(-occ // g.nx), 8)
    g.off = [min(i * g.rx, occ - g.rx) for i in range(g.nx)]
    g.wide = up(rows, SUB * LANE)
    g.own = max(g.wide, g.nz * g.lz)
    g.units = g.wide // LANE
    g.subs = g.units // SUB
    g.na = g.subs - 1
    g.slots = g.na + g.nx
    g.block = g.total // size_x
    g.per = size_x // size_y
    g.window = max(up(i * g.block % LANE + g.block, LANE) for i in range(g.per))
    g.wu = g.window // LANE
    g.firsts = [min(i * g.block // LANE * LANE, g.wide - g.window) for i in range(g.per)]
    g.begins = [i * g.block - g.firsts[i] for i in range(g.per)]
    g.odd = any(begin % 8 for begin in g.begins)
    g.share = occ // size_y
    g.j = up(g.share, 8)
    g.step = 512
    g.chunks = -(-depth // g.step)
    g.group = 512 if g.wide % 512 == 0 else 256
    return g


def flip(value, mask, size):
    if size & (size - 1):
        return lax.rem(value + mask, size)
    bit = 1
    while bit < size:
        if mask & bit:
            value = value + bit - 2 * bit * lax.rem(value // bit, 2)
        bit *= 2
    return value


def unflip(value, mask, size):
    return lax.rem(value - mask + size, size) if size & (size - 1) else flip(value, mask, size)


def greet(size_x, size_y):
    gx, gy = lax.axis_index("gx"), lax.axis_index("gy")
    barrier = pltpu.get_barrier_semaphore()

    def hello(step, carry):
        other = lax.rem(gx * size_y + gy + step, size_x * size_y)
        pl.semaphore_signal(
            barrier, inc=1, device_id=(other // size_y, lax.rem(other, size_y)), device_id_type=MESH
        )
        return carry

    lax.fori_loop(1, size_x * size_y, hello, 0)
    pl.semaphore_wait(barrier, size_x * size_y - 1)


def whole_kernel(g, names, *refs):
    r = types.SimpleNamespace(**dict(zip(names, refs)))
    nz, nx, ny, occ, rows = g.nz, g.nx, g.ny, g.occ, g.rows
    gx, gy = lax.axis_index("gx"), lax.axis_index("gy")
    z, x = gx // nx, lax.rem(gx, nx)
    y, c = gy // 2, lax.rem(gy, 2)
    partner = (gx, gy + 1 - 2 * c)

    def left(ref, sem):
        remote(ref, ref, sem, r.spare, partner).wait_send()

    loads = [pltpu.make_async_copy(r.orb_h, r.orbv, r.load_sem.at[0])]
    pieces = r.load_sem.shape[0] - 1
    tall = up(-(-g.depth // pieces), 8)
    for i in range(pieces):
        low, high = i * tall, min((i + 1) * tall, g.depth)
        loads.append(pltpu.make_async_copy(r.proj_h.at[low:high], r.projv.at[low:high], r.load_sem.at[i + 1]))
    for load in loads:
        load.start()
    span = SUB * LANE

    def int_load(s):
        low, high = s * span, min((s + 1) * span, rows)
        return pltpu.make_async_copy(r.int_h.at[0, low:high], r.integ.at[low:high], r.int_sem.at[s])

    greet(g.size_x, g.size_y)
    for load in loads:
        load.wait()
    for s in range(g.subs):
        int_load(s).start()

    def x_part(zz, w, e):
        to = lax.rem(x + e, nx)
        return remote(
            r.part.at[zz, w, to], r.xland.at[e - 1, zz, w], r.send_p, r.recv_p.at[zz, w, e - 1], (z * nx + to, gy)
        )

    tail = (rows - 1) // g.lz

    def put(zz, value):
        for w in range(g.waves):
            seg = value[:, w * LANE:(w + 1) * LANE].astype(BF16)
            if seg.shape[1]:
                for xx in range(nx):
                    r.part[zz, w, xx, :, :seg.shape[1]] = seg[g.off[xx]:g.off[xx] + g.rx]

    for d in reversed(range(nz)):
        zz = flip(z, d, nz)

        @pl.when(zz < tail)
        def _(zz=zz):
            put(zz, dot(r.orbv[...], r.projv[:, pl.ds(pl.multiple_of(zz * g.lz, LANE), g.lz)], ((1,), (0,))))

        @pl.when(zz == tail)
        def _():
            put(tail, dot(r.orbv[...], r.projv[:, tail * g.lz:rows], ((1,), (0,))))

        for w in range(g.waves):
            for e in range(1, nx):
                x_part(zz, w, e).start()

    def x_sum(zz, w):
        value = r.part[zz, w, x].astype(F32)
        for e in range(1, nx):
            x_part(zz, w, e).wait_recv()
            value = value + r.xland[e - 1, zz, w].astype(F32)
        return value

    def z_part(d, w):
        return remote(
            r.zsum.at[d - 1, w], r.zland.at[d - 1, w], r.send_q, r.recv_q.at[d - 1, w], (flip(z, d, nz) * nx + x, gy)
        )

    for d in reversed(range(1, nz)):
        for w in range(g.waves):
            r.zsum[d - 1, w] = x_sum(flip(z, d, nz), w).astype(BF16)
            z_part(d, w).start()

    def at(d, e):
        return unflip(z, d, nz) * nx + lax.rem(x - e + nx, nx)

    def group(f, core):
        return lax.rem(y - f + ny, ny) * 2 + core

    def block_up(k, w):
        ref = r.agb.at[gy, w, jnp.maximum(z - k, 0) * nx + x]
        return remote(ref, ref, r.send_au.at[k], r.recv_au.at[k, w], (jnp.minimum(z + 1, nz - 1) * nx + x, gy))

    def block_down(k, w):
        ref = r.agb.at[gy, w, jnp.minimum(z + k, nz - 1) * nx + x]
        return remote(ref, ref, r.send_ad.at[k], r.recv_ad.at[k, w], (jnp.maximum(z - 1, 0) * nx + x, gy))

    def block_came(zz, k, w, rising):
        ref = r.agb.at[gy, w, zz * nx + x]
        sem = r.recv_au if rising else r.recv_ad
        return remote(ref, ref, r.spare, sem.at[k - 1, w], partner)

    def block_x(gg, w, q, slot, e):
        ref = r.agb.at[gg, w, q]
        return remote(
            ref, ref, r.send_ax, r.recv_ax.at[slot, w, e - 1], (z * nx + lax.rem(x + e, nx), gy)
        )

    def block_y(gg, w, q, slot, f):
        ref = r.agb.at[gg, w, q]
        return remote(
            ref, ref, r.send_ay, r.recv_ay.at[slot, w, f - 1], (gx, lax.rem(y + f, ny) * 2 + c)
        )

    def block_c(f, zz, core):
        ref = r.agb.at[group(f, core), :, pl.ds(zz * nx, nx)]
        return remote(ref, ref, r.send_ac, r.recv_ac.at[f, zz], partner)

    for w in range(g.waves):
        total = x_sum(z, w)
        for d in range(1, nz):
            z_part(d, w).wait_recv()
            total = total + r.zland[d - 1, w].astype(F32)
        r.agb[gy, w, gx] = total.astype(BF16)

        @pl.when(z < nz - 1)
        def _(w=w):
            block_up(0, w).start()

        @pl.when(z > 0)
        def _(w=w):
            block_down(0, w).start()

        for e in range(1, nx):
            block_x(gy, w, gx, jnp.where(c == 0, z, z * ny), e).start()
        for f in range(1, ny):
            block_y(gy, w, gx, jnp.where(c == 0, z * nx, z), f).start()

    def planes(k, act):
        for rising in ((True, False) if k else (True,)):
            zz = z - k if rising else z + k

            @pl.when((zz >= 0) & (zz < nz))
            def _(zz=zz, rising=rising):
                act(jnp.clip(zz, 0, nz - 1), rising)

    def first_stage(k, x_first):
        def act(zz, rising):
            for w in range(g.waves):
                block_came(zz, k, w, rising).wait_recv()
                if k < nz - 1:
                    @pl.when((z < nz - 1) if rising else (z > 0))
                    def _():
                        (block_up if rising else block_down)(k, w).start()
                for e in range(1, nx):
                    block_x(gy, w, zz * nx + x, zz if x_first else zz * ny, e).start()
                for f in range(1, ny):
                    block_y(gy, w, zz * nx + x, zz * nx if x_first else zz, f).start()

        planes(k, act)

    def second_stage(k, x_first):
        def act(zz, rising):
            for w in range(g.waves):
                if x_first:
                    for e in range(1, nx):
                        q = zz * nx + lax.rem(x - e + nx, nx)
                        block_x(gy, w, q, zz, e).wait_recv()
                        for f in range(1, ny):
                            block_y(gy, w, q, zz * nx + e, f).start()
                else:
                    for f in range(1, ny):
                        block_y(group(f, c), w, zz * nx + x, zz, f).wait_recv()
                        for e in range(1, nx):
                            block_x(group(f, c), w, zz * nx + x, zz * ny + f, e).start()

        planes(k, act)

    def third_stage(k, x_first):
        def act(zz, rising):
            if x_first:
                block_c(0, zz, c).start()
            for f in range(1 if x_first else 0, ny):
                for w in range(g.waves):
                    if x_first:
                        for e in range(nx):
                            q = zz * nx + lax.rem(x - e + nx, nx)
                            block_y(group(f, c), w, q, zz * nx + e, f).wait_recv()
                    else:
                        for e in range(1, nx):
                            q = zz * nx + lax.rem(x - e + nx, nx)
                            block_x(group(f, c), w, q, zz * ny + f, e).wait_recv()
                block_c(f, zz, c).start()

        planes(k, act)

    for x_first in (True, False):
        @pl.when(c == (0 if x_first else 1))
        def _(x_first=x_first):
            for k in range(1, nz):
                first_stage(k, x_first)
                second_stage(k - 1, x_first)
                if k > 1:
                    third_stage(k - 2, x_first)
            second_stage(nz - 1, x_first)
            third_stage(nz - 2, x_first)
            third_stage(nz - 1, x_first)

    for f in range(ny):
        for zz in range(nz):
            block_c(f, zz, 1 - c).wait_recv()

    lane = lax.broadcasted_iota(jnp.int32, (g.rx, g.lz), 1)

    def joined(gg, q):
        return jnp.concatenate([r.agb[gg, w, q] for w in range(g.waves)], axis=1)

    for gg in range(g.size_y):
        for zz in range(nz):
            width = min(g.lz, rows - zz * g.lz)
            if width <= 0:
                continue
            base = gg * rows + zz * g.lz
            for xx in range(nx):
                r.admm[g.off[xx]:g.off[xx] + g.rx, base:base + width] = joined(gg, zz * nx + xx)[:, :width]
    for zz in range(nz):
        for xx in range(nx):
            piece = joined(gy, zz * nx + xx)
            piece = jnp.where(lane + zz * g.lz < rows, piece.astype(F32), 0.0).astype(BF16)
            r.own[g.off[xx]:g.off[xx] + g.rx, zz * g.lz:(zz + 1) * g.lz] = piece

    devices = g.size_x * g.size_y
    me = gx * g.size_y + gy
    root = gx // g.per
    root_y, root_c = root // 2, lax.rem(root, 2)
    turn = lax.rem(gx, g.per)
    first = 0
    for i in range(g.per):
        first = jnp.where(turn == i, g.firsts[i] // LANE, first)
    mine = gy == root
    below = (y != root_y) & (c == root_c)
    last = c != root_c

    def part_of(zz, slot):
        if slot < g.na:
            return r.cols.at[zz * nx + x, pl.ds(SUB * slot, SUB)]
        return r.cols.at[zz * nx + slot - g.na, pl.ds(SUB * g.na, SUB)]

    def upward(k, slot):
        ref = part_of(jnp.maximum(z - k, 0), slot)
        return remote(ref, ref, r.send_u.at[k], r.recv_u.at[k, slot], (jnp.minimum(z + 1, nz - 1) * nx + x, gy))

    def downward(k, slot):
        ref = part_of(jnp.minimum(z + k, nz - 1), slot)
        return remote(ref, ref, r.send_d.at[k], r.recv_d.at[k, slot], (jnp.maximum(z - 1, 0) * nx + x, gy))

    def sideways(zz, sub, e, came):
        ref = r.cols.at[zz * nx + (lax.rem(x - e + nx, nx) if came else x), pl.ds(SUB * sub, SUB)]
        return remote(
            ref, ref, r.send_x.at[zz], r.recv_x.at[zz, sub, e - 1], (z * nx + lax.rem(x + e, nx), gy)
        )

    def row_y(q, unit, f):
        spot = unit - first
        return remote(
            r.cols.at[q, unit], r.rows.at[q, spot], r.send_y.at[f - 1], r.recv_y.at[q], (gx, lax.rem(y + f, ny) * 2 + c)
        )

    def row_c(q, unit):
        spot = unit - first
        return remote(r.cols.at[q, unit], r.rows.at[q, spot], r.send_c, r.recv_c.at[q], partner)

    def row_all(q):
        return remote(r.rows.at[q], r.rows.at[q], r.send_w, r.recv_c.at[q], partner)

    def row_came(q):
        return remote(r.rows.at[q], r.rows.at[q], r.spare, r.recv_y.at[q], partner)

    def row_own(q):
        return pltpu.make_async_copy(r.cols.at[q, pl.ds(first, g.wu)], r.rows.at[q], r.row_sem.at[q])

    def pass_rows(q, sub):
        for h in range(SUB):
            unit = sub * SUB + h

            @pl.when(mine & (unit >= first) & (unit < first + g.wu))
            def _():
                for f in range(1, ny):
                    row_y(q, unit, f).start()
                row_c(q, unit).start()

    r.mixed[...] = jnp.zeros_like(r.mixed)
    r.trace[...] = jnp.zeros_like(r.trace)
    for s in range(g.subs):
        int_load(s).wait()
    spots = lax.broadcasted_iota(jnp.int32, (occ, span), 1)

    def half(i, carry):
        s = lax.rem(i + g.na, g.subs)
        start = pl.multiple_of(s * span, span)
        value = dot(r.admm[...], r.integ[pl.ds(start, span), :], ((1,), (1,)))
        value = jnp.where(spots + start < rows, value, 0.0)
        low = value.astype(BF16)
        for h in range(SUB):
            r.cols[gx, SUB * s + h] = low[:, h * LANE:(h + 1) * LANE]

        @pl.when(i == 0)
        def _():
            for e in range(1, nx):
                sideways(z, g.na, e, False).start()

        @pl.when(i > 0)
        def _():
            ref = r.cols.at[gx, pl.ds(SUB * s, SUB)]

            @pl.when(z < nz - 1)
            def _():
                remote(ref, ref, r.send_u.at[0], r.recv_u.at[0, s], (jnp.minimum(z + 1, nz - 1) * nx + x, gy)).start()

            @pl.when(z > 0)
            def _():
                remote(ref, ref, r.send_d.at[0], r.recv_d.at[0, s], (jnp.maximum(z - 1, 0) * nx + x, gy)).start()

            for e in range(1, nx):
                sideways(z, s, e, False).start()

        for h in range(SUB):
            unit = SUB * s + h

            @pl.when(mine & (unit >= first) & (unit < first + g.wu))
            def _():
                for f in range(1, ny):
                    row_y(gx, unit, f).start()
                row_c(gx, unit).start()

        exact = low.astype(F32)
        r.trace[...] += jnp.sum(exact * exact, axis=0, keepdims=True)
        r.mixed[...] += dot(r.own[:, pl.ds(start, span)], low, ((1,), (1,)))
        return carry

    lax.fori_loop(0, g.subs, half, 0)

    def z_send(k, slot):
        @pl.when((z >= k) & (z < nz - 1))
        def _():
            upward(k, slot).start()

        @pl.when((z + k < nz) & (z > 0))
        def _():
            downward(k, slot).start()

    for e in range(nx):
        for xx in range(nx):
            @pl.when(lax.rem(x - e + nx, nx) == xx)
            def _(e=e, xx=xx):
                if e > 0:
                    sideways(z, g.na, e, True).wait_recv()
                    pass_rows(z * nx + xx, g.na)
                z_send(0, g.na + xx)

    low = r.mixed[...].astype(BF16)
    row_i = lax.broadcasted_iota(jnp.int32, (g.j, occ), 0)
    col_i = lax.broadcasted_iota(jnp.int32, (g.j, occ), 1)
    for gg in range(g.size_y):
        pick = ((row_i < g.share) & (col_i == row_i + gg * g.share)).astype(F32).astype(BF16)
        r.mpart[gg] = dot(pick, low, ((1,), (0,))).astype(BF16)

    def mix_y(d):
        to = lax.rem(gy + d, g.size_y)
        return remote(r.mpart.at[to], r.mland.at[d - 1], r.send_m, r.recv_m.at[d - 1], (gx, to))

    for d in range(1, g.size_y):
        mix_y(d).start()
    total = r.mpart[gy].astype(F32)
    for d in range(1, g.size_y):
        mix_y(d).wait_recv()
        total = total + r.mland[d - 1].astype(F32)
    r.mall[gy, gx] = total.astype(BF16)

    def mix_z(d, came):
        ref = r.mall.at[gy, at(d, 0) if came else gx]
        return remote(ref, ref, r.send_n, r.recv_n.at[d - 1], (flip(z, d, nz) * nx + x, gy))

    def mix_x(d, e, came):
        ref = r.mall.at[gy, at(d, e if came else 0)]
        return remote(ref, ref, r.send_k, r.recv_k.at[d, e - 1], (z * nx + lax.rem(x + e, nx), gy))

    def mix_share(f, came):
        ref = r.mall.at[group(f, c) if came else gy]
        return remote(ref, ref, r.send_o, r.recv_o.at[f - 1], (gx, lax.rem(y + f, ny) * 2 + c))

    def mix_core(f, core):
        ref = r.mall.at[group(f, core)]
        return remote(ref, ref, r.send_r, r.recv_r.at[f], partner)

    for d in range(1, nz):
        mix_z(d, False).start()
    for e in range(1, nx):
        mix_x(0, e, False).start()
    stat_lane = lax.broadcasted_iota(jnp.int32, (1, LANE), 1)
    energy_part, trace_part = jnp.sum(total * total), jnp.sum(r.trace[...])
    r.stats[...] = jnp.where(stat_lane == 0, energy_part, jnp.where(stat_lane == 1, trace_part, 0.0))

    def stat_copy(to):
        return remote(r.stats, r.sland.at[me], r.send_s, r.recv_s, (to // g.size_y, lax.rem(to, g.size_y)))

    def tell(step, carry):
        stat_copy(lax.rem(me + step, devices)).start()
        return carry

    lax.fori_loop(1, devices, tell, 0)

    r.acc[...] = jnp.zeros_like(r.acc)
    r.applied[...] = jnp.zeros_like(r.applied)

    def units(ref, q, low, high):
        return jnp.concatenate([ref[q, u] for u in range(low, high)], axis=1)

    def exchange_term(zz):
        for xx in range(nx):
            q = zz * nx + xx

            @pl.when(mine)
            def _(q=q):
                row_own(q).wait()

            @pl.when(below)
            def _(q=q):
                row_came(q).wait_recv()
                row_all(q).start()

        @pl.when(last)
        def _():
            for xx in range(nx):
                row_all(zz * nx + xx).wait_recv()

        lefts = [units(r.rows, zz * nx + xx, 0, g.wu) for xx in range(nx)]
        for low in range(0, rows, g.group):
            high = min(low + g.group, rows)
            value = r.acc[:, low:high]
            for xx in range(nx):
                right = units(r.cols, zz * nx + xx, low // LANE, up(high, LANE) // LANE)[:, :high - low]
                value = value + dot(lefts[xx], right, ((0,), (0,)))
            r.acc[:, low:high] = value

    def applied_term(zz):
        value = r.applied[...]
        for xx in range(nx):
            q = zz * nx + xx
            left = jnp.concatenate([r.mall[gg, q] for gg in range(g.size_y)], axis=0)
            value = value + dot(left, units(r.cols, q, 0, g.units), ((1,), (0,)))
        r.applied[...] = value

    def level(k, act):
        def one(i, carry):
            zz = z - k + 2 * k * i

            @pl.when((zz >= 0) & (zz < nz))
            def _():
                act(zz)

            return carry

        lax.fori_loop(0, 2 if k else 1, one, 0)

    def arrive_x(k):
        for side in ((-1, 1) if k else (1,)):
            zz = z + side * k

            @pl.when((zz >= 0) & (zz < nz))
            def _(zz=zz):
                zz = jnp.clip(zz, 0, nz - 1)
                for sub in range(g.na):
                    for e in range(1, nx):
                        sideways(zz, sub, e, True).wait_recv()
                        pass_rows(zz * nx + lax.rem(x - e + nx, nx), sub)

        def own_rows(zz):
            @pl.when(mine)
            def _():
                for xx in range(nx):
                    row_own(zz * nx + xx).start()

        level(k, own_rows)

    def arrive_z(k, slot):
        for up_way in (True, False):
            zz = z - k if up_way else z + k

            @pl.when((zz >= 0) & (zz < nz))
            def _(zz=zz, up_way=up_way):
                zz = jnp.clip(zz, 0, nz - 1)
                sem = r.recv_u if up_way else r.recv_d
                ref = part_of(zz, slot)
                remote(ref, ref, r.spare, sem.at[k - 1, slot], partner).wait_recv()
                if k < nz - 1:
                    @pl.when((z < nz - 1) if up_way else (z > 0))
                    def _():
                        (upward if up_way else downward)(k, slot).start()
                if slot < g.na:
                    for e in range(1, nx):
                        sideways(zz, slot, e, False).start()
                    pass_rows(zz * nx + x, slot)
                else:
                    pass_rows(zz * nx + slot - g.na, g.na)

    def drain_first():
        left(r.xland, r.send_p)
        left(r.zland, r.send_q)
        for k in range(nz - 1):
            @pl.when((z >= k) & (z < nz - 1))
            def _(k=k):
                left(r.agb.at[0, :, 0], r.send_au.at[k])

            @pl.when((z + k < nz) & (z > 0))
            def _(k=k):
                left(r.agb.at[0, :, 0], r.send_ad.at[k])

        left(r.agb.at[0:ny], r.send_ac)

        @pl.when(c == 0)
        def _():
            left(r.agb.at[0, :, 0:nz * (nx - 1)], r.send_ax)
            left(r.agb.at[0:ny - 1], r.send_ay)

        @pl.when(c == 1)
        def _():
            left(r.agb.at[0:ny * (nx - 1) // nx], r.send_ax)
            left(r.agb.at[0, :, 0:nz * (ny - 1)], r.send_ay)

    def drain_mixed():
        left(r.mland, r.send_m)
        left(r.mall.at[0, 0:nz - 1], r.send_n)
        left(r.mall.at[0, 0:nz * (nx - 1)], r.send_k)
        left(r.mall.at[0:ny - 1], r.send_o)
        left(r.mall.at[0:ny], r.send_r)
        others = r.sland.at[0:devices - 1]
        remote(others, others, r.send_s, r.recv_s, partner).wait()
        r.sland[me] = r.stats[...]
        r.sums[...] = jnp.sum(r.sland[...], axis=0)

    def drain_level(k):
        span_of = r.cols.at[0:SUB, 0:g.slots]

        @pl.when((z >= k) & (z < nz - 1))
        def _():
            left(span_of, r.send_u.at[k])

        @pl.when((z + k < nz) & (z > 0))
        def _():
            left(span_of, r.send_d.at[k])

    def drain_x(k):
        def act(zz, rising):
            left(r.cols.at[0:nx - 1, 0:SUB * (g.na if k else g.subs)], r.send_x.at[zz])

        planes(k, act)

    edge = (z == 0) | (z == nz - 1)

    def share_mixed():
        for d in range(nz):
            for e in range(1, nx):
                mix_x(d, e, True).wait_recv()
        for f in range(1, ny):
            mix_share(f, False).start()
        mix_core(0, c).start()

    def work(k):
        if k < nz - 1:
            level(k - 1, exchange_term)
        else:
            for f in range(ny):
                mix_core(f, 1 - c).wait_recv()
            for j in range(nz - 2):
                level(j, applied_term)

            @pl.when(edge)
            def _():
                level(nz - 2, applied_term)

    for k in range(1, nz):
        for slot in range(g.slots):
            arrive_z(k, slot)
            if slot == 1:
                if k == 1:
                    drain_first()
                else:
                    drain_level(k - 2)
                    drain_x(k - 2)
            if slot == min(2, g.slots - 1):
                @pl.when(edge)
                def _(k=k):
                    arrive_x(k - 1)
            if slot == g.slots - 2:
                if k == 1:
                    for d in range(1, nz):
                        mix_z(d, True).wait_recv()
                        for e in range(1, nx):
                            mix_x(d, e, False).start()
                if k == nz - 1:
                    for f in range(1, ny):
                        mix_share(f, True).wait_recv()
                        mix_core(f, c).start()

                @pl.when(edge)
                def _(k=k):
                    work(k)

        @pl.when(jnp.logical_not(edge))
        def _(k=k):
            if k == nz - 1:
                work(k)
            arrive_x(k - 1)
            if k == nz - 2:
                share_mixed()
            if k < nz - 1:
                work(k)
            else:
                level(nz - 2, applied_term)

        if k == nz - 2:
            @pl.when(edge)
            def _():
                share_mixed()
    drain_mixed()
    arrive_x(nz - 1)
    drain_x(nz - 2)
    level(nz - 1, applied_term)

    low = r.applied[:, :rows].astype(BF16)

    def back_c(n, core):
        return remote(r.bpart.at[n, core], r.bland.at[n], r.send_v, r.recv_v.at[n], partner)

    def back_y(n, f):
        to = lax.rem(y + f, ny)
        return remote(r.bsum.at[n, to], r.byland.at[n, f - 1], r.send_b, r.recv_b.at[n, f - 1], (gx, to * 2 + c))

    def back_on(n):
        back_c(n, 1 - c).wait_recv()
        total = r.bpart[n, c].astype(F32) + r.bland[n].astype(F32)
        r.bsum[n] = total.astype(BF16)
        for f in range(1, ny):
            back_y(n, f).start()

    for n in range(g.chunks):
        start, stop = n * g.step, min((n + 1) * g.step, g.depth)
        value = dot(low, r.projv[start:stop, :], ((1,), (1,)))
        for gg in range(g.size_y):
            r.bpart[n, gg % 2, gg // 2, :, :stop - start] = value[gg * g.j:(gg + 1) * g.j].astype(BF16)
        back_c(n, 1 - c).start()
        if n > 0:
            back_on(n - 1)
    back_on(g.chunks - 1)
    level(nz - 2, exchange_term)
    level(nz - 1, exchange_term)
    if g.odd:
        result = pltpu.make_async_copy(r.acc, r.exch, r.out_sem)
    else:
        skip = 0
        for i in range(g.per):
            skip = jnp.where(turn == i, g.begins[i] // 8, skip)
        result = pltpu.make_async_copy(
            r.acc.at[pl.ds(pl.multiple_of(skip * 8, 8), g.block)], r.exch, r.out_sem
        )
    result.start()
    for n in range(g.chunks):
        total = r.bpart[n, c, y].astype(F32) + r.bland[n, y].astype(F32)
        for f in range(1, ny):
            back_y(n, f).wait_recv()
            total = total + r.byland[n, f - 1].astype(F32)
        start, stop = n * g.step, min((n + 1) * g.step, g.depth)
        r.back[:, start:stop] = total[:g.share, :stop - start]

    drain_level(nz - 2)
    drain_x(nz - 1)
    left(r.bland, r.send_v)
    left(r.byland, r.send_b)

    @pl.when(mine)
    def _():
        for f in range(1, ny):
            left(r.rows, r.send_y.at[f - 1])
        left(r.rows, r.send_c)

    @pl.when(below)
    def _():
        left(r.rows, r.send_w)

    result.wait()


def whole(g, orbitals, projector, integrals):
    dma, vmem = pltpu.SemaphoreType.DMA, pltpu.VMEM
    nz, nx, ny, occ = g.nz, g.nx, g.ny, g.occ
    devices = g.size_x * g.size_y
    scratch = dict(
        orbv=vmem(orbitals.shape, BF16),
        projv=vmem(projector.shape, BF16),
        integ=vmem((g.wide, g.total), BF16),
        part=vmem((nz, g.waves, nx, g.rx, LANE), BF16),
        xland=vmem((nx - 1, nz, g.waves, g.rx, LANE), BF16),
        zsum=vmem((nz - 1, g.waves, g.rx, LANE), BF16),
        zland=vmem((nz - 1, g.waves, g.rx, LANE), BF16),
        agb=vmem((g.size_y, g.waves, g.size_x, g.rx, LANE), BF16),
        admm=vmem((occ, g.total), BF16),
        own=vmem((occ, g.own), BF16),
        cols=vmem((g.size_x, g.units, occ, LANE), BF16),
        rows=vmem((g.size_x, g.wu, occ, LANE), BF16),
        acc=vmem((g.window, g.rows), F32),
        mixed=vmem((occ, occ), F32),
        out_sem=dma(()),
        trace=vmem((1, SUB * LANE), F32),
        mpart=vmem((g.size_y, g.j, occ), BF16),
        mland=vmem((g.size_y - 1, g.j, occ), BF16),
        mall=vmem((g.size_y, g.size_x, g.j, occ), BF16),
        stats=vmem((1, LANE), F32),
        sland=vmem((devices, 1, LANE), F32),
        applied=vmem((g.size_y * g.j, g.wide), F32),
        bpart=vmem((g.chunks, 2, ny, g.j, g.step), BF16),
        bland=vmem((g.chunks, ny, g.j, g.step), BF16),
        bsum=vmem((g.chunks, ny, g.j, g.step), BF16),
        byland=vmem((g.chunks, ny - 1, g.j, g.step), BF16),
        load_sem=dma((5,)),
        int_sem=dma((g.subs,)),
        row_sem=dma((g.size_x,)),
    )
    one = ()
    for letter, sends, arrivals in (
        ("p", one, (nz, g.waves, nx - 1)),
        ("q", one, (nz - 1, g.waves)),
        ("au", (nz - 1,), (nz - 1, g.waves)),
        ("ad", (nz - 1,), (nz - 1, g.waves)),
        ("ax", one, (nz * ny, g.waves, nx - 1)),
        ("ay", one, (nz * nx, g.waves, ny - 1)),
        ("ac", one, (ny, nz)),
        ("u", (nz - 1,), (nz - 1, g.slots)),
        ("d", (nz - 1,), (nz - 1, g.slots)),
        ("x", (nz,), (nz, g.subs, nx - 1)),
        ("m", one, (g.size_y - 1,)),
        ("n", one, (nz - 1,)),
        ("k", one, (nz, nx - 1)),
        ("o", one, (ny - 1,)),
        ("r", one, (ny,)),
        ("s", one, one),
        ("v", one, (g.chunks,)),
        ("b", one, (g.chunks, ny - 1)),
        ("y", (ny - 1,), (g.size_x,)),
        ("c", one, (g.size_x,)),
    ):
        scratch["send_" + letter] = dma(sends)
        scratch["recv_" + letter] = dma(arrivals)
    scratch.update(send_w=dma(one), spare=dma(one))
    names = ["orb_h", "proj_h", "int_h", "exch", "back", "sums"] + list(scratch)
    return pl.pallas_call(
        functools.partial(whole_kernel, g, names),
        out_shape=(
            vmem((g.window if g.odd else g.block, g.rows), F32),
            vmem((g.share, g.depth), F32),
            vmem((1, LANE), F32),
        ),
        in_specs=[pl.BlockSpec(memory_space=pl.ANY)] * 3,
        out_specs=[pl.BlockSpec(memory_space=pl.ANY)] + [pl.BlockSpec(memory_space=pltpu.VMEM)] * 2,
        scratch_shapes=list(scratch.values()),
        compiler_params=pltpu.CompilerParams(collective_id=1, has_side_effects=True, vmem_limit_bytes=LIMIT),
    )(orbitals, projector, integrals)


def finish_kernel(g, exch, back, sums, exch_o, back_o, energy, trace, sem, *spare):
    tall = up(-(-g.block // 8), 8)
    ready = exch
    if spare:
        ready = spare[0]
        turn = lax.rem(lax.axis_index("gx"), g.per)
        for i in range(g.per):
            @pl.when(turn == i)
            def _(i=i):
                ready[...] = exch[g.begins[i]:g.begins[i] + g.block, :]
    copies = [pltpu.make_async_copy(back, back_o, sem.at[0])]
    for i, low in enumerate(range(0, g.block, tall)):
        high = min(low + tall, g.block)
        copies.append(pltpu.make_async_copy(ready.at[low:high], exch_o.at[low:high], sem.at[i + 1]))
    for copy in copies:
        copy.start()
    lane = lax.broadcasted_iota(jnp.int32, (1, LANE), 1)
    value = sums[...]
    energy[...] = jnp.sum(jnp.where(lane == 0, value, 0.0), keepdims=True) * (-0.5 / (g.total * g.occ))
    trace[...] = jnp.sum(jnp.where(lane == 1, value, 0.0), keepdims=True) * (1.0 / g.total)
    for copy in copies:
        copy.wait()


def finish(g, exch, back, sums):
    vmem = pl.BlockSpec(memory_space=pltpu.VMEM)
    hbm = pl.BlockSpec(memory_space=pl.ANY)
    spare = [pltpu.VMEM((g.block, g.rows), F32)] if g.odd else []
    return pl.pallas_call(
        functools.partial(finish_kernel, g),
        out_shape=(
            jax.ShapeDtypeStruct((g.block, g.rows), F32),
            jax.ShapeDtypeStruct(back.shape, F32),
            jax.ShapeDtypeStruct((1, 1), F32),
            jax.ShapeDtypeStruct((1, 1), F32),
        ),
        in_specs=[vmem] * 3,
        out_specs=[hbm, hbm, vmem, vmem],
        scratch_shapes=[pltpu.SemaphoreType.DMA((9,))] + spare,
        compiler_params=pltpu.CompilerParams(vmem_limit_bytes=2 * 1024 * 1024 + 2 * (exch.size + back.size) * 4),
    )(exch, back, sums)


def on_device(size_x, size_y, orbitals, projector, integrals):
    g = layout(size_x, size_y, projector.shape[0], projector.shape[1], orbitals.shape[1])
    exchange, back, energy, trace = finish(g, *whole(g, orbitals.T, projector.T, integrals))
    return (exchange, back.T, energy.reshape(()), trace.reshape(()))


def solution(mesh):
    return jax.shard_map(
        functools.partial(on_device, mesh.shape["gx"], mesh.shape["gy"]),
        mesh=mesh,
        in_specs=(P("gx", None), P("gy", "gx"), P("gx", "gy", None)),
        out_specs=(P("gx", "gy"), P("gx", "gy"), P(), P()),
        check_vma=False,
    )
```

```python
import functools
import types

import jax
import jax.numpy as jnp
from jax import lax
from jax.experimental import pallas as pl
from jax.experimental.pallas import tpu as pltpu
from jax.sharding import PartitionSpec as P

MESH = pl.DeviceIdType.MESH
LIMIT = 57 * 1024 * 1024
LANE = 128
SUB = 2
F32, BF16 = jnp.float32, jnp.bfloat16


def factor(size):
    inner = 1
    while inner * inner * 4 <= size:
        inner *= 2
    return size // inner, inner


def up(value, unit):
    return -(-value // unit) * unit


def remote(src, dst, send, recv, dev):
    return pltpu.make_async_remote_copy(
        src_ref=src, dst_ref=dst, send_sem=send, recv_sem=recv, device_id=dev, device_id_type=MESH
    )


def dot(a, b, dims):
    return lax.dot_general(a, b, (dims, ((), ())), preferred_element_type=F32)


def layout(size_x, size_y, rows, depth, occ):
    g = types.SimpleNamespace(size_x=size_x, size_y=size_y, rows=rows, depth=depth, occ=occ)
    g.nz, g.nx = factor(size_x)
    g.ny = size_y // 2
    g.total = rows * size_y
    g.lz = up(-(-rows // g.nz), LANE)
    g.waves = g.lz // LANE
    g.rx = up(-(-occ // g.nx), 8)
    g.off = [min(i * g.rx, occ - g.rx) for i in range(g.nx)]
    g.wide = up(rows, SUB * LANE)
    g.own = max(g.wide, g.nz * g.lz)
    g.units = g.wide // LANE
    g.subs = g.units // SUB
    g.na = g.subs - 1
    g.slots = g.na + g.nx
    g.block = g.total // size_x
    g.per = size_x // size_y
    g.window = max(up(i * g.block % LANE + g.block, LANE) for i in range(g.per))
    g.wu = g.window // LANE
    g.firsts = [min(i * g.block // LANE * LANE, g.wide - g.window) for i in range(g.per)]
    g.begins = [i * g.block - g.firsts[i] for i in range(g.per)]
    g.odd = any(begin % 8 for begin in g.begins)
    g.share = occ // size_y
    g.j = up(g.share, 8)
    g.step = 512
    g.chunks = -(-depth // g.step)
    g.group = 512 if g.wide % 512 == 0 else 256
    return g


def flip(value, mask, size):
    if size & (size - 1):
        return lax.rem(value + mask, size)
    bit = 1
    while bit < size:
        if mask & bit:
            value = value + bit - 2 * bit * lax.rem(value // bit, 2)
        bit *= 2
    return value


def unflip(value, mask, size):
    return lax.rem(value - mask + size, size) if size & (size - 1) else flip(value, mask, size)


def greet(size_x, size_y):
    gx, gy = lax.axis_index("gx"), lax.axis_index("gy")
    barrier = pltpu.get_barrier_semaphore()

    def hello(step, carry):
        other = lax.rem(gx * size_y + gy + step, size_x * size_y)
        pl.semaphore_signal(
            barrier, inc=1, device_id=(other // size_y, lax.rem(other, size_y)), device_id_type=MESH
        )
        return carry

    lax.fori_loop(1, size_x * size_y, hello, 0)
    return barrier


def whole_kernel(g, names, *refs):
    r = types.SimpleNamespace(**dict(zip(names, refs)))
    nz, nx, ny, occ, rows = g.nz, g.nx, g.ny, g.occ, g.rows
    gx, gy = lax.axis_index("gx"), lax.axis_index("gy")
    z, x = gx // nx, lax.rem(gx, nx)
    y, c = gy // 2, lax.rem(gy, 2)
    partner = (gx, gy + 1 - 2 * c)

    def left(ref, sem):
        remote(ref, ref, sem, r.spare, partner).wait_send()

    loads = [pltpu.make_async_copy(r.orb_h, r.orbv, r.load_sem.at[0])]
    tail = (rows - 1) // g.lz

    def piece_load(d, last_one):
        low, high = tail * g.lz, rows
        if not last_one:
            low, high = pl.multiple_of(flip(z, d, nz) * g.lz, LANE), None
        cut = pl.ds(low, g.lz if high is None else high - low)
        return pltpu.make_async_copy(r.proj_h.at[:, cut], r.projv.at[:, cut], r.load_sem.at[d + 1])

    def on_piece(d, act):
        @pl.when(flip(z, d, nz) < tail)
        def _():
            act(piece_load(d, False))

        @pl.when(flip(z, d, nz) == tail)
        def _():
            act(piece_load(d, True))

    loads[0].start()
    for d in reversed(range(nz)):
        on_piece(d, lambda copy: copy.start())
    span = SUB * LANE

    def int_load(s):
        low, high = s * span, min((s + 1) * span, rows)
        return pltpu.make_async_copy(r.int_h.at[0, low:high], r.integ.at[low:high], r.int_sem.at[s])

    barrier = greet(g.size_x, g.size_y)
    loads[0].wait()

    def x_part(zz, w, e):
        to = lax.rem(x + e, nx)
        return remote(
            r.part.at[zz, w, to], r.xland.at[e - 1, zz, w], r.send_p, r.recv_p.at[zz, w, e - 1], (z * nx + to, gy)
        )

    def put(zz, value):
        for w in range(g.waves):
            seg = value[:, w * LANE:(w + 1) * LANE].astype(BF16)
            if seg.shape[1]:
                for xx in range(nx):
                    r.part[zz, w, xx, :, :seg.shape[1]] = seg[g.off[xx]:g.off[xx] + g.rx]

    for d in reversed(range(nz)):
        zz = flip(z, d, nz)
        on_piece(d, lambda copy: copy.wait())
        if d == 0:
            for s in range(g.subs):
                int_load(s).start()

        @pl.when(zz < tail)
        def _(zz=zz):
            put(zz, dot(r.orbv[...], r.projv[:, pl.ds(pl.multiple_of(zz * g.lz, LANE), g.lz)], ((1,), (0,))))

        @pl.when(zz == tail)
        def _():
            put(tail, dot(r.orbv[...], r.projv[:, tail * g.lz:rows], ((1,), (0,))))

        if d == nz - 1:
            pl.semaphore_wait(barrier, g.size_x * g.size_y - 1)
        for w in range(g.waves):
            for e in range(1, nx):
                x_part(zz, w, e).start()

    def x_sum(zz, w):
        value = r.part[zz, w, x].astype(F32)
        for e in range(1, nx):
            x_part(zz, w, e).wait_recv()
            value = value + r.xland[e - 1, zz, w].astype(F32)
        return value

    def z_part(d, w):
        return remote(
            r.zsum.at[d - 1, w], r.zland.at[d - 1, w], r.send_q, r.recv_q.at[d - 1, w], (flip(z, d, nz) * nx + x, gy)
        )

    for d in reversed(range(1, nz)):
        for w in range(g.waves):
            r.zsum[d - 1, w] = x_sum(flip(z, d, nz), w).astype(BF16)
            z_part(d, w).start()

    def at(d, e):
        return unflip(z, d, nz) * nx + lax.rem(x - e + nx, nx)

    def group(f, core):
        return lax.rem(y - f + ny, ny) * 2 + core

    def block_up(k, w):
        ref = r.agb.at[gy, w, jnp.maximum(z - k, 0) * nx + x]
        return remote(ref, ref, r.send_au.at[k], r.recv_au.at[k, w], (jnp.minimum(z + 1, nz - 1) * nx + x, gy))

    def block_down(k, w):
        ref = r.agb.at[gy, w, jnp.minimum(z + k, nz - 1) * nx + x]
        return remote(ref, ref, r.send_ad.at[k], r.recv_ad.at[k, w], (jnp.maximum(z - 1, 0) * nx + x, gy))

    def block_came(zz, k, w, rising):
        ref = r.agb.at[gy, w, zz * nx + x]
        sem = r.recv_au if rising else r.recv_ad
        return remote(ref, ref, r.spare, sem.at[k - 1, w], partner)

    def block_x(gg, w, q, slot, e):
        ref = r.agb.at[gg, w, q]
        return remote(
            ref, ref, r.send_ax, r.recv_ax.at[slot, w, e - 1], (z * nx + lax.rem(x + e, nx), gy)
        )

    def block_y(gg, w, q, slot, f):
        ref = r.agb.at[gg, w, q]
        return remote(
            ref, ref, r.send_ay, r.recv_ay.at[slot, w, f - 1], (gx, lax.rem(y + f, ny) * 2 + c)
        )

    def block_c(f, zz, core):
        ref = r.agb.at[group(f, core), :, pl.ds(zz * nx, nx)]
        return remote(ref, ref, r.send_ac, r.recv_ac.at[f, zz], partner)

    for w in range(g.waves):
        total = x_sum(z, w)
        for d in range(1, nz):
            z_part(d, w).wait_recv()
            total = total + r.zland[d - 1, w].astype(F32)
        r.agb[gy, w, gx] = total.astype(BF16)

        @pl.when(z < nz - 1)
        def _(w=w):
            block_up(0, w).start()

        @pl.when(z > 0)
        def _(w=w):
            block_down(0, w).start()

        for e in range(1, nx):
            block_x(gy, w, gx, jnp.where(c == 0, z, z * ny), e).start()
        for f in range(1, ny):
            block_y(gy, w, gx, jnp.where(c == 0, z * nx, z), f).start()

    def planes(k, act):
        for rising in ((True, False) if k else (True,)):
            zz = z - k if rising else z + k

            @pl.when((zz >= 0) & (zz < nz))
            def _(zz=zz, rising=rising):
                act(jnp.clip(zz, 0, nz - 1), rising)

    def first_stage(k, x_first):
        def act(zz, rising):
            for w in range(g.waves):
                block_came(zz, k, w, rising).wait_recv()
                if k < nz - 1:
                    @pl.when((z < nz - 1) if rising else (z > 0))
                    def _():
                        (block_up if rising else block_down)(k, w).start()
                for e in range(1, nx):
                    block_x(gy, w, zz * nx + x, zz if x_first else zz * ny, e).start()
                for f in range(1, ny):
                    block_y(gy, w, zz * nx + x, zz * nx if x_first else zz, f).start()

        planes(k, act)

    def second_stage(k, x_first):
        def act(zz, rising):
            for w in range(g.waves):
                if x_first:
                    for e in range(1, nx):
                        q = zz * nx + lax.rem(x - e + nx, nx)
                        block_x(gy, w, q, zz, e).wait_recv()
                        for f in range(1, ny):
                            block_y(gy, w, q, zz * nx + e, f).start()
                else:
                    for f in range(1, ny):
                        block_y(group(f, c), w, zz * nx + x, zz, f).wait_recv()
                        for e in range(1, nx):
                            block_x(group(f, c), w, zz * nx + x, zz * ny + f, e).start()

        planes(k, act)

    def third_stage(k, x_first):
        def act(zz, rising):
            if x_first:
                block_c(0, zz, c).start()
            for f in range(1 if x_first else 0, ny):
                for w in range(g.waves):
                    if x_first:
                        for e in range(nx):
                            q = zz * nx + lax.rem(x - e + nx, nx)
                            block_y(group(f, c), w, q, zz * nx + e, f).wait_recv()
                    else:
                        for e in range(1, nx):
                            q = zz * nx + lax.rem(x - e + nx, nx)
                            block_x(group(f, c), w, q, zz * ny + f, e).wait_recv()
                block_c(f, zz, c).start()

        planes(k, act)

    for x_first in (True, False):
        @pl.when(c == (0 if x_first else 1))
        def _(x_first=x_first):
            for k in range(1, nz):
                first_stage(k, x_first)
                second_stage(k - 1, x_first)
                if k > 1:
                    third_stage(k - 2, x_first)
            second_stage(nz - 1, x_first)
            third_stage(nz - 2, x_first)
            third_stage(nz - 1, x_first)

    for f in range(ny):
        for zz in range(nz):
            block_c(f, zz, 1 - c).wait_recv()

    lane = lax.broadcasted_iota(jnp.int32, (g.rx, g.lz), 1)

    def joined(gg, q):
        return jnp.concatenate([r.agb[gg, w, q] for w in range(g.waves)], axis=1)

    for gg in range(g.size_y):
        for zz in range(nz):
            width = min(g.lz, rows - zz * g.lz)
            if width <= 0:
                continue
            base = gg * rows + zz * g.lz
            for xx in range(nx):
                r.admm[g.off[xx]:g.off[xx] + g.rx, base:base + width] = joined(gg, zz * nx + xx)[:, :width]
    devices = g.size_x * g.size_y
    me = gx * g.size_y + gy
    root = gx // g.per
    root_y, root_c = root // 2, lax.rem(root, 2)
    turn = lax.rem(gx, g.per)
    first = 0
    for i in range(g.per):
        first = jnp.where(turn == i, g.firsts[i] // LANE, first)
    mine = gy == root
    below = (y != root_y) & (c == root_c)
    last = c != root_c

    def part_of(zz, slot):
        if slot < g.na:
            return r.cols.at[zz * nx + x, pl.ds(SUB * slot, SUB)]
        return r.cols.at[zz * nx + slot - g.na, pl.ds(SUB * g.na, SUB)]

    def upward(k, slot):
        ref = part_of(jnp.maximum(z - k, 0), slot)
        return remote(ref, ref, r.send_u.at[k], r.recv_u.at[k, slot], (jnp.minimum(z + 1, nz - 1) * nx + x, gy))

    def downward(k, slot):
        ref = part_of(jnp.minimum(z + k, nz - 1), slot)
        return remote(ref, ref, r.send_d.at[k], r.recv_d.at[k, slot], (jnp.maximum(z - 1, 0) * nx + x, gy))

    def sideways(zz, sub, e, came):
        ref = r.cols.at[zz * nx + (lax.rem(x - e + nx, nx) if came else x), pl.ds(SUB * sub, SUB)]
        return remote(
            ref, ref, r.send_x.at[zz], r.recv_x.at[zz, sub, e - 1], (z * nx + lax.rem(x + e, nx), gy)
        )

    def row_y(q, unit, f):
        spot = unit - first
        return remote(
            r.cols.at[q, unit], r.rows.at[q, spot], r.send_y.at[f - 1], r.recv_y.at[q], (gx, lax.rem(y + f, ny) * 2 + c)
        )

    def row_c(q, unit):
        spot = unit - first
        return remote(r.cols.at[q, unit], r.rows.at[q, spot], r.send_c, r.recv_c.at[q], partner)

    def row_all(q):
        return remote(r.rows.at[q], r.rows.at[q], r.send_w, r.recv_c.at[q], partner)

    def row_came(q):
        return remote(r.rows.at[q], r.rows.at[q], r.spare, r.recv_y.at[q], partner)

    def row_own(q):
        return pltpu.make_async_copy(r.cols.at[q, pl.ds(first, g.wu)], r.rows.at[q], r.row_sem.at[q])

    def pass_rows(q, sub):
        for h in range(SUB):
            unit = sub * SUB + h

            @pl.when(mine & (unit >= first) & (unit < first + g.wu))
            def _():
                for f in range(1, ny):
                    row_y(q, unit, f).start()
                row_c(q, unit).start()

    for s in range(g.subs):
        int_load(s).wait()
    spots = lax.broadcasted_iota(jnp.int32, (occ, span), 1)

    def half(i, carry):
        s = lax.rem(i + g.na, g.subs)
        start = pl.multiple_of(s * span, span)
        value = dot(r.admm[...], r.integ[pl.ds(start, span), :], ((1,), (1,)))
        value = jnp.where(spots + start < rows, value, 0.0)
        low = value.astype(BF16)
        for h in range(SUB):
            r.cols[gx, SUB * s + h] = low[:, h * LANE:(h + 1) * LANE]

        @pl.when(i == 0)
        def _():
            for e in range(1, nx):
                sideways(z, g.na, e, False).start()

        @pl.when(i > 0)
        def _():
            ref = r.cols.at[gx, pl.ds(SUB * s, SUB)]

            @pl.when(z < nz - 1)
            def _():
                remote(ref, ref, r.send_u.at[0], r.recv_u.at[0, s], (jnp.minimum(z + 1, nz - 1) * nx + x, gy)).start()

            @pl.when(z > 0)
            def _():
                remote(ref, ref, r.send_d.at[0], r.recv_d.at[0, s], (jnp.maximum(z - 1, 0) * nx + x, gy)).start()

            for e in range(1, nx):
                sideways(z, s, e, False).start()

        for h in range(SUB):
            unit = SUB * s + h

            @pl.when(mine & (unit >= first) & (unit < first + g.wu))
            def _():
                for f in range(1, ny):
                    row_y(gx, unit, f).start()
                row_c(gx, unit).start()

        return carry

    lax.fori_loop(0, g.subs, half, 0)

    def z_send(k, slot):
        @pl.when((z >= k) & (z < nz - 1))
        def _():
            upward(k, slot).start()

        @pl.when((z + k < nz) & (z > 0))
        def _():
            downward(k, slot).start()

    for e in range(nx):
        for xx in range(nx):
            @pl.when(lax.rem(x - e + nx, nx) == xx)
            def _(e=e, xx=xx):
                if e > 0:
                    sideways(z, g.na, e, True).wait_recv()
                    pass_rows(z * nx + xx, g.na)
                z_send(0, g.na + xx)

    for zz in range(nz):
        for xx in range(nx):
            piece = joined(gy, zz * nx + xx)
            piece = jnp.where(lane + zz * g.lz < rows, piece.astype(F32), 0.0).astype(BF16)
            r.own[g.off[xx]:g.off[xx] + g.rx, zz * g.lz:(zz + 1) * g.lz] = piece
    halves = jnp.concatenate([r.cols[gx, u] for u in range(g.units)], axis=1)
    exact = halves.astype(F32)
    r.trace[...] = jnp.sum(exact * exact, axis=0, keepdims=True)
    low = dot(r.own[:, :g.wide], halves, ((1,), (1,))).astype(BF16)
    row_i = lax.broadcasted_iota(jnp.int32, (g.j, occ), 0)
    col_i = lax.broadcasted_iota(jnp.int32, (g.j, occ), 1)
    for gg in range(g.size_y):
        pick = ((row_i < g.share) & (col_i == row_i + gg * g.share)).astype(F32).astype(BF16)
        r.mpart[gg] = dot(pick, low, ((1,), (0,))).astype(BF16)

    def mix_y(d):
        to = lax.rem(gy + d, g.size_y)
        return remote(r.mpart.at[to], r.mland.at[d - 1], r.send_m, r.recv_m.at[d - 1], (gx, to))

    for d in range(1, g.size_y):
        mix_y(d).start()
    total = r.mpart[gy].astype(F32)
    for d in range(1, g.size_y):
        mix_y(d).wait_recv()
        total = total + r.mland[d - 1].astype(F32)
    r.mall[gy, gx] = total.astype(BF16)

    def mix_z(d, came):
        ref = r.mall.at[gy, at(d, 0) if came else gx]
        return remote(ref, ref, r.send_n, r.recv_n.at[d - 1], (flip(z, d, nz) * nx + x, gy))

    def mix_x(d, e, came):
        ref = r.mall.at[gy, at(d, e if came else 0)]
        return remote(ref, ref, r.send_k, r.recv_k.at[d, e - 1], (z * nx + lax.rem(x + e, nx), gy))

    def mix_share(f, came):
        ref = r.mall.at[group(f, c) if came else gy]
        return remote(ref, ref, r.send_o, r.recv_o.at[f - 1], (gx, lax.rem(y + f, ny) * 2 + c))

    def mix_core(f, core):
        ref = r.mall.at[group(f, core)]
        return remote(ref, ref, r.send_r, r.recv_r.at[f], partner)

    for d in range(1, nz):
        mix_z(d, False).start()
    for e in range(1, nx):
        mix_x(0, e, False).start()
    stat_lane = lax.broadcasted_iota(jnp.int32, (1, LANE), 1)
    energy_part, trace_part = jnp.sum(total * total), jnp.sum(r.trace[...])
    r.stats[...] = jnp.where(stat_lane == 0, energy_part, jnp.where(stat_lane == 1, trace_part, 0.0))

    def stat_copy(to):
        return remote(r.stats, r.sland.at[me], r.send_s, r.recv_s, (to // g.size_y, lax.rem(to, g.size_y)))

    def tell(step, carry):
        stat_copy(lax.rem(me + step, devices)).start()
        return carry

    lax.fori_loop(1, devices, tell, 0)

    r.acc[...] = jnp.zeros_like(r.acc)
    r.applied[...] = jnp.zeros_like(r.applied)

    def units(ref, q, low, high):
        return jnp.concatenate([ref[q, u] for u in range(low, high)], axis=1)

    def forward_rows(zz):
        @pl.when(below)
        def _():
            for xx in range(nx):
                row_came(zz * nx + xx).wait_recv()
                row_all(zz * nx + xx).start()

    def exchange_term(zz):
        @pl.when(mine)
        def _():
            for xx in range(nx):
                row_own(zz * nx + xx).wait()

        @pl.when(last)
        def _():
            for xx in range(nx):
                row_all(zz * nx + xx).wait_recv()

        lefts = [units(r.rows, zz * nx + xx, 0, g.wu) for xx in range(nx)]
        for low in range(0, rows, g.group):
            high = min(low + g.group, rows)
            value = r.acc[:, low:high]
            for xx in range(nx):
                right = units(r.cols, zz * nx + xx, low // LANE, up(high, LANE) // LANE)[:, :high - low]
                value = value + dot(lefts[xx], right, ((0,), (0,)))
            r.acc[:, low:high] = value

    def applied_term(zz):
        value = r.applied[...]
        for xx in range(nx):
            q = zz * nx + xx
            left = jnp.concatenate([r.mall[gg, q] for gg in range(g.size_y)], axis=0)
            value = value + dot(left, units(r.cols, q, 0, g.units), ((1,), (0,)))
        r.applied[...] = value

    def level(k, act):
        def one(i, carry):
            zz = z - k + 2 * k * i

            @pl.when((zz >= 0) & (zz < nz))
            def _():
                act(zz)

            return carry

        lax.fori_loop(0, 2 if k else 1, one, 0)

    def arrive_x(k):
        for side in ((-1, 1) if k else (1,)):
            zz = z + side * k

            @pl.when((zz >= 0) & (zz < nz))
            def _(zz=zz):
                zz = jnp.clip(zz, 0, nz - 1)
                for sub in range(g.na):
                    for e in range(1, nx):
                        sideways(zz, sub, e, True).wait_recv()
                        pass_rows(zz * nx + lax.rem(x - e + nx, nx), sub)

        def own_rows(zz):
            @pl.when(mine)
            def _():
                for xx in range(nx):
                    row_own(zz * nx + xx).start()

        level(k, own_rows)

    def arrive_z(k, slot):
        for up_way in (True, False):
            zz = z - k if up_way else z + k

            @pl.when((zz >= 0) & (zz < nz))
            def _(zz=zz, up_way=up_way):
                zz = jnp.clip(zz, 0, nz - 1)
                sem = r.recv_u if up_way else r.recv_d
                ref = part_of(zz, slot)
                remote(ref, ref, r.spare, sem.at[k - 1, slot], partner).wait_recv()
                if k < nz - 1:
                    @pl.when((z < nz - 1) if up_way else (z > 0))
                    def _():
                        (upward if up_way else downward)(k, slot).start()
                if slot < g.na:
                    for e in range(1, nx):
                        sideways(zz, slot, e, False).start()
                    pass_rows(zz * nx + x, slot)
                else:
                    pass_rows(zz * nx + slot - g.na, g.na)

    def drain_first():
        left(r.xland, r.send_p)
        left(r.zland, r.send_q)
        for k in range(nz - 1):
            @pl.when((z >= k) & (z < nz - 1))
            def _(k=k):
                left(r.agb.at[0, :, 0], r.send_au.at[k])

            @pl.when((z + k < nz) & (z > 0))
            def _(k=k):
                left(r.agb.at[0, :, 0], r.send_ad.at[k])

        left(r.agb.at[0:ny], r.send_ac)

        @pl.when(c == 0)
        def _():
            left(r.agb.at[0, :, 0:nz * (nx - 1)], r.send_ax)
            left(r.agb.at[0:ny - 1], r.send_ay)

        @pl.when(c == 1)
        def _():
            left(r.agb.at[0:ny * (nx - 1) // nx], r.send_ax)
            left(r.agb.at[0, :, 0:nz * (ny - 1)], r.send_ay)

    def drain_mixed():
        left(r.mland, r.send_m)
        left(r.mall.at[0, 0:nz - 1], r.send_n)
        left(r.mall.at[0, 0:nz * (nx - 1)], r.send_k)
        left(r.mall.at[0:ny - 1], r.send_o)
        left(r.mall.at[0:ny], r.send_r)
        others = r.sland.at[0:devices - 1]
        remote(others, others, r.send_s, r.recv_s, partner).wait()
        r.sland[me] = r.stats[...]
        r.sums[...] = jnp.sum(r.sland[...], axis=0)

    def drain_level(k):
        span_of = r.cols.at[0:SUB, 0:g.slots]

        @pl.when((z >= k) & (z < nz - 1))
        def _():
            left(span_of, r.send_u.at[k])

        @pl.when((z + k < nz) & (z > 0))
        def _():
            left(span_of, r.send_d.at[k])

    def drain_x(k):
        def act(zz, rising):
            left(r.cols.at[0:nx - 1, 0:SUB * (g.na if k else g.subs)], r.send_x.at[zz])

        planes(k, act)

    edge = (z == 0) | (z == nz - 1)

    def share_mixed():
        for d in range(nz):
            for e in range(1, nx):
                mix_x(d, e, True).wait_recv()
        for f in range(1, ny):
            mix_share(f, False).start()
        mix_core(0, c).start()

    def work(k):
        if k < nz - 1:
            level(k - 1, forward_rows)
            level(k - 1, exchange_term)
        else:
            for f in range(ny):
                mix_core(f, 1 - c).wait_recv()
            for j in range(nz - 2):
                level(j, applied_term)

            @pl.when(edge)
            def _():
                level(nz - 2, applied_term)

    for k in range(1, nz):
        for slot in range(g.slots):
            arrive_z(k, slot)
            if slot == 1:
                if k == 1:
                    drain_first()
                else:
                    drain_level(k - 2)
                    drain_x(k - 2)
            if slot == min(2, g.slots - 1):
                @pl.when(edge)
                def _(k=k):
                    arrive_x(k - 1)
            if slot == g.slots - 2:
                if k == 1:
                    for d in range(1, nz):
                        mix_z(d, True).wait_recv()
                        for e in range(1, nx):
                            mix_x(d, e, False).start()
                if k == nz - 1:
                    for f in range(1, ny):
                        mix_share(f, True).wait_recv()
                        mix_core(f, c).start()

                @pl.when(edge)
                def _(k=k):
                    work(k)

        @pl.when(jnp.logical_not(edge))
        def _(k=k):
            if k == nz - 1:
                work(k)
            arrive_x(k - 1)
            if k == nz - 2:
                share_mixed()
            if k < nz - 1:
                work(k)
            else:
                level(nz - 2, applied_term)

        if k == nz - 2:
            @pl.when(edge)
            def _():
                share_mixed()
    drain_mixed()
    arrive_x(nz - 1)
    drain_x(nz - 2)
    level(nz - 1, applied_term)

    low = r.applied[:, :rows].astype(BF16)

    def back_c(n, core):
        return remote(r.bpart.at[n, core], r.bland.at[n], r.send_v, r.recv_v.at[n], partner)

    def back_y(n, f):
        to = lax.rem(y + f, ny)
        return remote(r.bsum.at[n, to], r.byland.at[n, f - 1], r.send_b, r.recv_b.at[n, f - 1], (gx, to * 2 + c))

    def back_on(n):
        back_c(n, 1 - c).wait_recv()
        total = r.bpart[n, c].astype(F32) + r.bland[n].astype(F32)
        r.bsum[n] = total.astype(BF16)
        for f in range(1, ny):
            back_y(n, f).start()

    for n in range(g.chunks):
        start, stop = n * g.step, min((n + 1) * g.step, g.depth)
        value = dot(low, r.projv[start:stop, :], ((1,), (1,)))
        for gg in range(g.size_y):
            r.bpart[n, gg % 2, gg // 2, :, :stop - start] = value[gg * g.j:(gg + 1) * g.j].astype(BF16)
        back_c(n, 1 - c).start()
        if n > 0:
            back_on(n - 1)
        if n == min(2, g.chunks - 1):
            level(nz - 2, forward_rows)
    back_on(g.chunks - 1)
    level(nz - 1, forward_rows)
    level(nz - 2, exchange_term)
    level(nz - 1, exchange_term)
    if g.odd:
        result = pltpu.make_async_copy(r.acc, r.exch, r.out_sem)
    else:
        skip = 0
        for i in range(g.per):
            skip = jnp.where(turn == i, g.begins[i] // 8, skip)
        result = pltpu.make_async_copy(
            r.acc.at[pl.ds(pl.multiple_of(skip * 8, 8), g.block)], r.exch, r.out_sem
        )
    result.start()
    for n in range(g.chunks):
        total = r.bpart[n, c, y].astype(F32) + r.bland[n, y].astype(F32)
        for f in range(1, ny):
            back_y(n, f).wait_recv()
            total = total + r.byland[n, f - 1].astype(F32)
        start, stop = n * g.step, min((n + 1) * g.step, g.depth)
        r.back[:, start:stop] = total[:g.share, :stop - start]

    drain_level(nz - 2)
    drain_x(nz - 1)
    left(r.bland, r.send_v)
    left(r.byland, r.send_b)

    @pl.when(mine)
    def _():
        for f in range(1, ny):
            left(r.rows, r.send_y.at[f - 1])
        left(r.rows, r.send_c)

    @pl.when(below)
    def _():
        left(r.rows, r.send_w)

    result.wait()


def whole(g, orbitals, projector, integrals):
    dma, vmem = pltpu.SemaphoreType.DMA, pltpu.VMEM
    nz, nx, ny, occ = g.nz, g.nx, g.ny, g.occ
    devices = g.size_x * g.size_y
    scratch = dict(
        orbv=vmem(orbitals.shape, BF16),
        projv=vmem(projector.shape, BF16),
        integ=vmem((g.wide, g.total), BF16),
        part=vmem((nz, g.waves, nx, g.rx, LANE), BF16),
        xland=vmem((nx - 1, nz, g.waves, g.rx, LANE), BF16),
        zsum=vmem((nz - 1, g.waves, g.rx, LANE), BF16),
        zland=vmem((nz - 1, g.waves, g.rx, LANE), BF16),
        agb=vmem((g.size_y, g.waves, g.size_x, g.rx, LANE), BF16),
        admm=vmem((occ, g.total), BF16),
        own=vmem((occ, g.own), BF16),
        cols=vmem((g.size_x, g.units, occ, LANE), BF16),
        rows=vmem((g.size_x, g.wu, occ, LANE), BF16),
        acc=vmem((g.window, g.rows), F32),
        out_sem=dma(()),
        trace=vmem((1, g.wide), F32),
        mpart=vmem((g.size_y, g.j, occ), BF16),
        mland=vmem((g.size_y - 1, g.j, occ), BF16),
        mall=vmem((g.size_y, g.size_x, g.j, occ), BF16),
        stats=vmem((1, LANE), F32),
        sland=vmem((devices, 1, LANE), F32),
        applied=vmem((g.size_y * g.j, g.wide), F32),
        bpart=vmem((g.chunks, 2, ny, g.j, g.step), BF16),
        bland=vmem((g.chunks, ny, g.j, g.step), BF16),
        bsum=vmem((g.chunks, ny, g.j, g.step), BF16),
        byland=vmem((g.chunks, ny - 1, g.j, g.step), BF16),
        load_sem=dma((nz + 1,)),
        int_sem=dma((g.subs,)),
        row_sem=dma((g.size_x,)),
    )
    one = ()
    for letter, sends, arrivals in (
        ("p", one, (nz, g.waves, nx - 1)),
        ("q", one, (nz - 1, g.waves)),
        ("au", (nz - 1,), (nz - 1, g.waves)),
        ("ad", (nz - 1,), (nz - 1, g.waves)),
        ("ax", one, (nz * ny, g.waves, nx - 1)),
        ("ay", one, (nz * nx, g.waves, ny - 1)),
        ("ac", one, (ny, nz)),
        ("u", (nz - 1,), (nz - 1, g.slots)),
        ("d", (nz - 1,), (nz - 1, g.slots)),
        ("x", (nz,), (nz, g.subs, nx - 1)),
        ("m", one, (g.size_y - 1,)),
        ("n", one, (nz - 1,)),
        ("k", one, (nz, nx - 1)),
        ("o", one, (ny - 1,)),
        ("r", one, (ny,)),
        ("s", one, one),
        ("v", one, (g.chunks,)),
        ("b", one, (g.chunks, ny - 1)),
        ("y", (ny - 1,), (g.size_x,)),
        ("c", one, (g.size_x,)),
    ):
        scratch["send_" + letter] = dma(sends)
        scratch["recv_" + letter] = dma(arrivals)
    scratch.update(send_w=dma(one), spare=dma(one))
    names = ["orb_h", "proj_h", "int_h", "exch", "back", "sums"] + list(scratch)
    return pl.pallas_call(
        functools.partial(whole_kernel, g, names),
        out_shape=(
            vmem((g.window if g.odd else g.block, g.rows), F32),
            vmem((g.share, g.depth), F32),
            vmem((1, LANE), F32),
        ),
        in_specs=[pl.BlockSpec(memory_space=pl.ANY)] * 3,
        out_specs=[pl.BlockSpec(memory_space=pl.ANY)] + [pl.BlockSpec(memory_space=pltpu.VMEM)] * 2,
        scratch_shapes=list(scratch.values()),
        compiler_params=pltpu.CompilerParams(collective_id=1, has_side_effects=True, vmem_limit_bytes=LIMIT),
    )(orbitals, projector, integrals)


def finish_kernel(g, exch, back, sums, exch_o, back_o, energy, trace, sem, *spare):
    tall = up(-(-g.block // 8), 8)
    ready = exch
    if spare:
        ready = spare[0]
        turn = lax.rem(lax.axis_index("gx"), g.per)
        for i in range(g.per):
            @pl.when(turn == i)
            def _(i=i):
                ready[...] = exch[g.begins[i]:g.begins[i] + g.block, :]
    copies = [pltpu.make_async_copy(back, back_o, sem.at[0])]
    for i, low in enumerate(range(0, g.block, tall)):
        high = min(low + tall, g.block)
        copies.append(pltpu.make_async_copy(ready.at[low:high], exch_o.at[low:high], sem.at[i + 1]))
    for copy in copies:
        copy.start()
    lane = lax.broadcasted_iota(jnp.int32, (1, LANE), 1)
    value = sums[...]
    energy[...] = jnp.sum(jnp.where(lane == 0, value, 0.0), keepdims=True) * (-0.5 / (g.total * g.occ))
    trace[...] = jnp.sum(jnp.where(lane == 1, value, 0.0), keepdims=True) * (1.0 / g.total)
    for copy in copies:
        copy.wait()


def finish(g, exch, back, sums):
    vmem = pl.BlockSpec(memory_space=pltpu.VMEM)
    hbm = pl.BlockSpec(memory_space=pl.ANY)
    spare = [pltpu.VMEM((g.block, g.rows), F32)] if g.odd else []
    return pl.pallas_call(
        functools.partial(finish_kernel, g),
        out_shape=(
            jax.ShapeDtypeStruct((g.block, g.rows), F32),
            jax.ShapeDtypeStruct(back.shape, F32),
            jax.ShapeDtypeStruct((1, 1), F32),
            jax.ShapeDtypeStruct((1, 1), F32),
        ),
        in_specs=[vmem] * 3,
        out_specs=[hbm, hbm, vmem, vmem],
        scratch_shapes=[pltpu.SemaphoreType.DMA((9,))] + spare,
        compiler_params=pltpu.CompilerParams(vmem_limit_bytes=2 * 1024 * 1024 + 2 * (exch.size + back.size) * 4),
    )(exch, back, sums)


def on_device(size_x, size_y, orbitals, projector, integrals):
    g = layout(size_x, size_y, projector.shape[0], projector.shape[1], orbitals.shape[1])
    exchange, back, energy, trace = finish(g, *whole(g, orbitals.T, projector.T, integrals))
    return (exchange, back.T, energy.reshape(()), trace.reshape(()))


def solution(mesh):
    return jax.shard_map(
        functools.partial(on_device, mesh.shape["gx"], mesh.shape["gy"]),
        mesh=mesh,
        in_specs=(P("gx", None), P("gy", "gx"), P("gx", "gy", None)),
        out_specs=(P("gx", "gy"), P("gx", "gy"), P(), P()),
        check_vma=False,
    )
```
